64 devices in a mesh: dp: 4 (over x, y), tp: 16 (over z, core).
Axes of the slice: x: 2, y: 2, z: 8, core: 2. Of those that a mesh axis runs over, the one named last changes fastest.
The devices are a block of a 4x4x8 slice.
Arguments:
- k_cache: bfloat16 [64, 16, 1024, 128], P('dp', None, 'tp'), parts along dimension 0
- v_cache: bfloat16 [64, 16, 1024, 128], P('dp', None, 'tp'), parts along dimension 0
- prompt_len: int32 [64], P('dp'), parts along dimension 0
- x_steps: bfloat16 [64, 64, 2048], P(None, 'dp'), parts along dimension 1
- w_norm: bfloat16 [2048], replicated
- w_q: bfloat16 [2048, 2048], P(None, 'tp')
- w_k: bfloat16 [2048, 2048], P(None, 'tp')
- w_v: bfloat16 [2048, 2048], P(None, 'tp')
- w_o: bfloat16 [2048, 2048], P('tp')
Outputs:
- output 1: bfloat16 [64, 64, 2048], P(None, 'dp'), parts along dimension 1
- output 2: bfloat16 [64, 16, 1088, 128], P('dp', 'tp'), parts along dimension 0
- output 3: bfloat16 [64, 16, 1088, 128], P('dp', 'tp'), parts along dimension 0
There are 4 independent parts. The reference program is written for one: setup_inputs(seed, part) draws one part's arguments, and reference() takes and returns one part's arrays. A program takes and returns all parts, laid end to end along the dimension named above; an argument that names none is the same for every part.
All inputs are finite; a program needn't handle non-finite values.
Results may differ from the reference program's by a relative error of at most 0.0196691.
Values are sent between devices in bfloat16 or wider.
A program may use at most 768 MiB of HBM per device.

```python
import jax
import jax.numpy as jnp
from jax import lax

MODEL_DIM = 2048
NUM_HEADS = 16
HEAD_DIM = 128
BATCH_ROWS = 16
SEQ_LEN = 1024
DECODE_STEPS = 64


def rotate(values, positions):
    half_dim = HEAD_DIM // 2
    inv_freq = 10000.0 ** (-2.0 * jnp.arange(half_dim, dtype=jnp.float32) / HEAD_DIM)
    angles = positions.astype(jnp.float32)[..., None] * inv_freq
    cos_part = jnp.cos(angles)
    sin_part = jnp.sin(angles)
    first_half = values[..., :half_dim]
    second_half = values[..., half_dim:]
    return jnp.concatenate([first_half * cos_part - second_half * sin_part, second_half * cos_part + first_half * sin_part], axis=-1)


def setup_inputs(seed: int = 0, part: int = 0) -> dict:
    part_key = jax.random.fold_in(jax.random.key(seed), part)
    draw_keys = jax.random.split(part_key, 6)
    shared_keys = jax.random.split(jax.random.key(seed + 1), 5)
    proj_width = NUM_HEADS * HEAD_DIM
    cache_shape = (BATCH_ROWS, NUM_HEADS, SEQ_LEN, HEAD_DIM)
    k_cache = jax.random.normal(draw_keys[0], cache_shape, jnp.float32).astype(jnp.bfloat16)
    v_cache = jax.random.normal(draw_keys[1], cache_shape, jnp.float32).astype(jnp.bfloat16)
    half_len = SEQ_LEN // 2
    lengths = jax.random.randint(draw_keys[2], (BATCH_ROWS,), half_len, SEQ_LEN + 1)
    long_row = jax.random.randint(draw_keys[3], (), 0, BATCH_ROWS)
    short_row = (long_row + jax.random.randint(draw_keys[4], (), 1, BATCH_ROWS)) % BATCH_ROWS
    row_ids = jnp.arange(BATCH_ROWS)
    lengths = jnp.where(row_ids == long_row, SEQ_LEN, lengths)
    lengths = jnp.where(row_ids == short_row, half_len, lengths)
    x_steps = jax.random.normal(draw_keys[5], (DECODE_STEPS, BATCH_ROWS, MODEL_DIM), jnp.float32).astype(jnp.bfloat16)
    w_norm = (0.5 * jax.random.normal(shared_keys[0], (MODEL_DIM,), jnp.float32)).astype(jnp.bfloat16)
    in_scale = MODEL_DIM ** -0.5
    w_q = (in_scale * jax.random.normal(shared_keys[1], (MODEL_DIM, proj_width), jnp.float32)).astype(jnp.bfloat16)
    w_k = (in_scale * jax.random.normal(shared_keys[2], (MODEL_DIM, proj_width), jnp.float32)).astype(jnp.bfloat16)
    w_v = (in_scale * jax.random.normal(shared_keys[3], (MODEL_DIM, proj_width), jnp.float32)).astype(jnp.bfloat16)
    out_scale = (SEQ_LEN / (4.0 * proj_width)) ** 0.5
    w_o = (out_scale * jax.random.normal(shared_keys[4], (proj_width, MODEL_DIM), jnp.float32)).astype(jnp.bfloat16)
    return {"k_cache": k_cache, "v_cache": v_cache, "prompt_len": lengths.astype(jnp.int32), "x_steps": x_steps, "w_norm": w_norm, "w_q": w_q, "w_k": w_k, "w_v": w_v, "w_o": w_o}


def reference(k_cache, v_cache, prompt_len, x_steps, w_norm, w_q, w_k, w_v, w_o):
    out_len = SEQ_LEN + DECODE_STEPS
    q_scale = HEAD_DIM ** -0.5
    norm_gain = 1.0 + w_norm.astype(jnp.float32)
    zero_tail = jnp.zeros((BATCH_ROWS, NUM_HEADS, DECODE_STEPS, HEAD_DIM), jnp.float32)
    keys_init = jnp.concatenate([k_cache.astype(jnp.float32), zero_tail], axis=2)
    vals_init = jnp.concatenate([v_cache.astype(jnp.float32), zero_tail], axis=2)
    slot_ids = jnp.arange(out_len)

    def write_row(cache_row, new_row, start_slot):
        return lax.dynamic_update_slice(cache_row, new_row, (0, start_slot, 0))

    def project(normed, weight):
        proj_flat = jnp.dot(normed, weight, preferred_element_type=jnp.float32).astype(jnp.bfloat16)
        return proj_flat.reshape(BATCH_ROWS, NUM_HEADS, HEAD_DIM).astype(jnp.float32)

    def step(state_in, step_in):
        keys_all, vals_all = state_in
        x_step, step_idx = step_in
        residual = x_step.astype(jnp.float32)
        inv_rms = lax.rsqrt(jnp.mean(residual * residual, axis=-1, keepdims=True) + 1e-6)
        normed = (residual * inv_rms * norm_gain).astype(jnp.bfloat16)
        position = prompt_len + step_idx
        queries = (rotate(project(normed, w_q), position[:, None]) * q_scale).astype(jnp.bfloat16).astype(jnp.float32)
        key_new = rotate(project(normed, w_k), position[:, None]).astype(jnp.bfloat16).astype(jnp.float32)
        val_new = project(normed, w_v)
        keys_all = jax.vmap(write_row)(keys_all, key_new[:, :, None, :], position)
        vals_all = jax.vmap(write_row)(vals_all, val_new[:, :, None, :], position)
        scores = jnp.einsum("bhd,bhtd->bht", queries, keys_all)
        is_valid = (slot_ids[None, :] <= position[:, None])[:, None, :]
        scores = jnp.where(is_valid, scores, -jnp.inf)
        row_peak = jnp.max(scores, axis=-1, keepdims=True)
        exp_scores = jnp.exp(scores - row_peak)
        attn_probs = (exp_scores / jnp.sum(exp_scores, axis=-1, keepdims=True)).astype(jnp.bfloat16).astype(jnp.float32)
        heads_out = jnp.einsum("bht,bhtd->bhd", attn_probs, vals_all).astype(jnp.bfloat16)
        attn_part = jnp.dot(heads_out.reshape(BATCH_ROWS, NUM_HEADS * HEAD_DIM), w_o, preferred_element_type=jnp.float32)
        return (keys_all, vals_all), (residual + attn_part).astype(jnp.bfloat16)

    final_state, y_steps = lax.scan(step, (keys_init, vals_init), (x_steps, jnp.arange(DECODE_STEPS)))
    return y_steps, final_state[0].astype(jnp.bfloat16), final_state[1].astype(jnp.bfloat16)
```

```python
import functools

import jax
import jax.numpy as jnp
from jax import lax
from jax.experimental import pallas as pl
from jax.experimental.pallas import tpu as pltpu
from jax.sharding import PartitionSpec as P

ROPE_BASE = 10000.0
NORM_EPS = 1e-6
CORES = 2
GROUP_ROWS = 2
PIECES = 4
X_STEPS = 8
MESH = pl.DeviceIdType.MESH
BF16 = jnp.bfloat16
F32 = jnp.float32


def main_kernel(n_tp, plen, freq, k_in, v_in, x_in, gain, w_q, w_k, w_v, w_o, k_buf, v_buf, y_buf,
                wq_v, wk_v, wv_v, x_blk, qkv, q_s, k_n, v_n, o_sr, o_snd, o_all, w_col, x_res,
                in_sem, x_sem, send_sem, recv_sem, w_send, w_recv, p_send, p_recv,
                o_send, o_recv, y_send, y_recv, d_send, d_recv):
    num_rows, out_len, head_dim = k_buf.shape
    n_steps, _, model_dim = x_in.shape
    slots = k_in.shape[2]
    seq_len = slots * n_tp
    chips = n_tp // CORES
    far = chips // 2
    half_steps = n_steps // CORES
    half_rows = half_steps * num_rows
    piece = half_rows // PIECES
    wide = CORES * head_dim
    n_groups = num_rows // GROUP_ROWS

    dp = lax.axis_index("dp")
    me = lax.axis_index("tp")
    chip = me // CORES
    core = lax.rem(me, CORES)
    other = 1 - core

    def chip_at(offset):
        return lax.rem(chip + offset + chips, chips)

    def device(chip_index, core_index):
        return (dp, chip_index * CORES + core_index)

    partner = device(chip, other)

    barrier = pltpu.get_barrier_semaphore()
    offsets = [0] + [s * d for d in range(1, far) for s in (1, -1)] + [far]
    for off in offsets:
        for c in range(CORES):
            if (off, c) != (0, 0):
                pl.semaphore_signal(barrier, inc=1, device_id=device(chip_at(off), lax.rem(core + c, CORES)), device_id_type=MESH)

    loads = [
        pltpu.make_async_copy(w_q, wq_v, in_sem.at[0]),
        pltpu.make_async_copy(w_k, wk_v, in_sem.at[1]),
        pltpu.make_async_copy(w_v, wv_v, in_sem.at[2]),
        pltpu.make_async_copy(
            x_in.at[pl.ds(core * half_steps, half_steps), :, pl.ds(pl.multiple_of(chip * wide, wide), wide)], x_res, in_sem.at[3]),
        pltpu.make_async_copy(
            w_o.at[:, pl.ds(pl.multiple_of(chip * wide, wide), wide)],
            w_col.at[chip, pl.ds(pl.multiple_of(core * head_dim, head_dim), head_dim)], in_sem.at[4]),
    ]
    for load in loads:
        load.start()

    def x_load(i, slot):
        return pltpu.make_async_copy(x_in.at[pl.ds(i * X_STEPS, X_STEPS)], x_blk.at[slot], x_sem.at[slot])

    x_load(0, 0).start()

    pl.semaphore_wait(barrier, n_tp - 1)

    my_slots = pl.ds(pl.multiple_of(me * slots, slots), slots)

    def send_group(i, _):
        rows = pl.ds(i * GROUP_ROWS, GROUP_ROWS)
        for which, (src, dst) in enumerate(((k_in, k_buf), (v_in, v_buf))):
            pltpu.make_async_copy(src.at[rows, me], dst.at[rows, my_slots], recv_sem.at[which, i]).start()
            for off in reversed(offsets):
                for c in range(CORES):
                    if (off, c) != (0, 0):
                        to_core = lax.rem(core + c, CORES)
                        to_chip = chip_at(off)
                        pltpu.make_async_remote_copy(
                            src_ref=src.at[rows, to_chip * CORES + to_core],
                            dst_ref=dst.at[rows, my_slots],
                            send_sem=send_sem.at[which, i],
                            recv_sem=recv_sem.at[which, i],
                            device_id=device(to_chip, to_core),
                            device_id_type=MESH,
                        ).start()
        return 0

    lax.fori_loop(0, n_groups, send_group, 0)

    w_copies = []
    for i, off in enumerate(reversed(offsets[1:])):
        to_chip = chip_at(off)
        w_copies.append(pltpu.make_async_remote_copy(
            src_ref=w_o.at[:, pl.ds(pl.multiple_of(to_chip * wide, wide), wide)],
            dst_ref=w_col.at[chip, pl.ds(pl.multiple_of(core * head_dim, head_dim), head_dim)],
            send_sem=w_send.at[i],
            recv_sem=w_recv.at[i],
            device_id=device(to_chip, core),
            device_id_type=MESH,
        ))
        w_copies[-1].start()

    for load in loads[:3]:
        load.wait()
    n_blocks = n_steps // X_STEPS
    blk_rows = X_STEPS * num_rows

    def project(i, _):
        slot = lax.rem(i, 2)

        @pl.when(i + 1 < n_blocks)
        def _():
            x_load(i + 1, 1 - slot).start()

        x_load(i, slot).wait()
        x = x_blk[slot].reshape(blk_rows, model_dim).astype(F32)
        inv = lax.rsqrt(jnp.mean(x * x, axis=-1, keepdims=True) + NORM_EPS)
        normed = (x * inv * (1.0 + gain[...].astype(F32))).astype(BF16)
        out = pl.ds(pl.multiple_of(i * blk_rows, blk_rows), blk_rows)
        for j, w in enumerate((wq_v, wk_v, wv_v)):
            qkv[j, out, :] = jnp.dot(normed, w[...], preferred_element_type=F32).astype(BF16).astype(F32)
        return 0

    lax.fori_loop(0, n_blocks, project, 0)

    def rope_row(b, _):
        step_id = lax.broadcasted_iota(jnp.int32, (n_steps, head_dim), 0)
        angle = (step_id + plen[b]).astype(F32) * freq[...]
        lane = lax.broadcasted_iota(jnp.int32, (n_steps, head_dim), 1)
        cos_part = jnp.cos(angle)
        sin_part = jnp.where(lane < head_dim // 2, -1.0, 1.0) * jnp.sin(angle)
        row = pl.ds(b, n_steps, stride=num_rows)

        def rotate(u):
            return u * cos_part + pltpu.roll(u, head_dim // 2, 1) * sin_part

        q_s[b] = (rotate(qkv[0, row, :]) * head_dim ** -0.5).astype(BF16)
        k_n[b] = rotate(qkv[1, row, :]).astype(BF16)
        v_n[b] = qkv[2, row, :].astype(BF16)
        for buf in (k_buf, v_buf):
            buf[b, seq_len:, :] = jnp.zeros((out_len - seq_len, head_dim), BF16)
        return 0

    lax.fori_loop(0, num_rows, rope_row, 0)

    def attend_row(b):
        start = plen[b]
        slot_id = lax.broadcasted_iota(jnp.int32, (out_len, n_steps), 0)
        step_id = lax.broadcasted_iota(jnp.int32, (out_len, n_steps), 1)
        pick = jnp.where(slot_id - step_id == start, 1.0, 0.0).astype(BF16)
        at = lax.broadcasted_iota(jnp.int32, (out_len, head_dim), 0) - start
        is_new = jnp.logical_and(at >= 0, at < n_steps)
        for buf, new in ((k_buf, k_n), (v_buf, v_n)):
            placed = jnp.dot(pick, new[b], preferred_element_type=F32)
            buf[b] = jnp.where(is_new, placed, buf[b].astype(F32)).astype(BF16)
        s = lax.dot_general(q_s[b], k_buf[b], (((1,), (1,)), ((), ())), preferred_element_type=F32)
        s_slot = lax.broadcasted_iota(jnp.int32, (n_steps, out_len), 1)
        s_step = lax.broadcasted_iota(jnp.int32, (n_steps, out_len), 0)
        s = jnp.where(s_slot - s_step <= start, s, -jnp.inf)
        e = jnp.exp(s - jnp.max(s, axis=-1, keepdims=True))
        a = (e / jnp.sum(e, axis=-1, keepdims=True)).astype(BF16)
        o = jnp.dot(a, v_buf[b], preferred_element_type=F32)
        o_sr[pl.ds(b, n_steps, stride=num_rows), :] = o.astype(BF16).astype(F32)

    def attend_group(i, _):
        rows = pl.ds(i * GROUP_ROWS, GROUP_ROWS)
        for which, buf in enumerate((k_buf, v_buf)):
            got = buf.at[rows, pl.ds(0, seq_len)]
            pltpu.make_async_copy(got, got, recv_sem.at[which, i]).wait()
        for r in range(GROUP_ROWS):
            attend_row(i * GROUP_ROWS + r)
        return 0

    lax.fori_loop(0, n_groups, attend_group, 0)

    my_lanes = pl.ds(pl.multiple_of(core * head_dim, head_dim), head_dim)
    mine = pl.ds(pl.multiple_of(core * half_rows, half_rows), half_rows)
    theirs = pl.ds(pl.multiple_of(other * half_rows, half_rows), half_rows)
    o_snd[...] = o_sr[theirs, :].astype(BF16)
    swap = pltpu.make_async_remote_copy(
        src_ref=o_snd, dst_ref=o_all.at[chip, :, my_lanes], send_sem=p_send.at[0], recv_sem=p_recv.at[0],
        device_id=partner, device_id_type=MESH)
    swap.start()
    o_all[chip, :, my_lanes] = o_sr[mine, :].astype(BF16)

    loads[3].wait()
    loads[4].wait()
    for copy in w_copies:
        copy.wait()
    w_swap = pltpu.make_async_remote_copy(
        src_ref=w_col.at[:, my_lanes], dst_ref=w_col.at[:, my_lanes], send_sem=p_send.at[1], recv_sem=p_recv.at[1],
        device_id=partner, device_id_type=MESH)
    w_swap.start()
    swap.wait()

    def hops(way, j):
        return far if (way + j) % 2 == 0 else far - 1

    def ring_copy(at, sems, way, hop, j):
        step = 1 if way == 0 else -1
        view = at(chip_at(-step * (hop - 1)), j)
        return pltpu.make_async_remote_copy(
            src_ref=view, dst_ref=view, send_sem=sems[0].at[way, hop - 1, j], recv_sem=sems[1].at[way, hop - 1, j],
            device_id=device(chip_at(step), core), device_id_type=MESH)

    def o_at(c, j):
        return o_all.at[c, pl.ds(j * piece, piece)]

    def y_at(c, j):
        return y_buf.at[pl.ds(pl.multiple_of(core * half_rows, half_rows) + j * piece, piece), pl.ds(pl.multiple_of(c * wide, wide), wide)]

    def hand_on(c, j):
        return pltpu.make_async_remote_copy(
            src_ref=y_at(c, j), dst_ref=y_at(c, j), send_sem=d_send.at[j], recv_sem=d_recv.at[j],
            device_id=partner, device_id_type=MESH)

    o_sems, y_sems = (o_send, o_recv), (y_send, y_recv)
    for j in range(PIECES):
        for way in range(2):
            ring_copy(o_at, o_sems, way, 1, j).start()

    def block_of_y(j):
        acc = x_res[j * (piece // num_rows):(j + 1) * (piece // num_rows)].reshape(piece, wide).astype(F32)
        total = jnp.zeros((piece, wide), F32)
        for c in range(chips):
            total += jnp.dot(o_all[c, j * piece:(j + 1) * piece, :], w_col[c], preferred_element_type=F32)
        y_buf[pl.ds(pl.multiple_of(core * half_rows, half_rows) + j * piece, piece), pl.ds(pl.multiple_of(chip * wide, wide), wide)] = (acc + total).astype(BF16)
        for way in range(2):
            ring_copy(y_at, y_sems, way, 1, j).start()
        hand_on(chip, j).start()

    for hop in range(1, far + 1):
        for j in range(PIECES):
            for way in range(2):
                if hop <= hops(way, j):
                    ring_copy(o_at, o_sems, way, hop, j).wait_recv()
                    if hop < hops(way, j):
                        ring_copy(o_at, o_sems, way, hop + 1, j).start()
            if hop == far:
                if j == 0:
                    w_swap.wait()
                block_of_y(j)
    for hop in range(1, far + 1):
        for j in range(PIECES):
            for way in range(2):
                if hop <= hops(way, j):
                    ring_copy(y_at, y_sems, way, hop, j).wait_recv()
                    if hop < hops(way, j):
                        ring_copy(y_at, y_sems, way, hop + 1, j).start()
                    hand_on(chip_at(-hop if way == 0 else hop), j).start()

    for i in range(n_groups):
        rows = pl.ds(i * GROUP_ROWS, GROUP_ROWS)
        for which, buf in enumerate((k_buf, v_buf)):
            sent = buf.at[rows, pl.ds(0, seq_len - slots)]
            pltpu.make_async_copy(sent, sent, send_sem.at[which, i]).wait()
    for hop in range(1, far + 1):
        for j in range(PIECES):
            for way in range(2):
                if hop <= hops(way, j):
                    ring_copy(o_at, o_sems, way, hop, j).wait_send()
                    ring_copy(y_at, y_sems, way, hop, j).wait_send()
    for j in range(PIECES):
        sent = y_buf.at[pl.ds(pl.multiple_of(core * half_rows, half_rows) + j * piece, piece)]
        pltpu.make_async_copy(sent, sent, d_send.at[j]).wait()
        got = y_buf.at[pl.ds(pl.multiple_of(other * half_rows, half_rows) + j * piece, piece)]
        pltpu.make_async_copy(got, got, d_recv.at[j]).wait()


def write_kernel(k_buf, v_buf, y_buf, k_out, v_out, y_out, sem):
    copies = [
        pltpu.make_async_copy(k_buf, k_out, sem.at[0]),
        pltpu.make_async_copy(v_buf, v_out, sem.at[1]),
        pltpu.make_async_copy(y_buf, y_out, sem.at[2]),
    ]
    for copy in copies:
        copy.start()
    for copy in copies:
        copy.wait()


def solution(mesh):
    n_tp = mesh.shape["tp"]

    def local_block(k_cache, v_cache, prompt_len, x_steps, w_norm, w_q, w_k, w_v, w_o):
        num_rows, _, slots, head_dim = k_cache.shape
        n_steps, _, model_dim = x_steps.shape
        out_len = slots * n_tp + n_steps
        chips = n_tp // CORES
        far = chips // 2
        half_rows = n_steps // CORES * num_rows
        wide = CORES * head_dim
        n_groups = num_rows // GROUP_ROWS
        lanes = jnp.arange(head_dim, dtype=jnp.int32) % (head_dim // 2)
        freq = (ROPE_BASE ** (-2.0 * lanes.astype(F32) / head_dim)).reshape(1, head_dim)
        dma = pltpu.SemaphoreType.DMA
        any_space = pl.BlockSpec(memory_space=pl.ANY)
        vmem = pl.BlockSpec(memory_space=pltpu.VMEM)
        cache = jax.ShapeDtypeStruct((num_rows, out_len, head_dim), BF16)
        k_buf, v_buf, y_buf = pl.pallas_call(
            functools.partial(main_kernel, n_tp),
            out_shape=(cache, cache, jax.ShapeDtypeStruct((n_steps * num_rows, model_dim), BF16)),
            in_specs=[pl.BlockSpec(memory_space=pltpu.SMEM), vmem, any_space, any_space, any_space, vmem] + [any_space] * 4,
            out_specs=(vmem, vmem, vmem),
            scratch_shapes=[
                pltpu.VMEM((model_dim, head_dim), BF16),
                pltpu.VMEM((model_dim, head_dim), BF16),
                pltpu.VMEM((model_dim, head_dim), BF16),
                pltpu.VMEM((2, X_STEPS, num_rows, model_dim), BF16),
                pltpu.VMEM((3, n_steps * num_rows, head_dim), F32),
                pltpu.VMEM((num_rows, n_steps, head_dim), BF16),
                pltpu.VMEM((num_rows, n_steps, head_dim), BF16),
                pltpu.VMEM((num_rows, n_steps, head_dim), BF16),
                pltpu.VMEM((n_steps * num_rows, head_dim), F32),
                pltpu.VMEM((half_rows, head_dim), BF16),
                pltpu.VMEM((chips, half_rows, wide), BF16),
                pltpu.VMEM((chips, wide, wide), BF16),
                pltpu.VMEM((n_steps // CORES, num_rows, wide), BF16),
                dma((5,)), dma((2,)),
                dma((2, n_groups)), dma((2, n_groups)),
                dma((chips - 1,)), dma((chips - 1,)),
                dma((2,)), dma((2,)),
                dma((2, far, PIECES)), dma((2, far, PIECES)),
                dma((2, far, PIECES)), dma((2, far, PIECES)),
                dma((PIECES,)), dma((PIECES,)),
            ],
            compiler_params=pltpu.CompilerParams(collective_id=0, has_side_effects=True, vmem_limit_bytes=44 * 2**20),
            name="decode_block",
        )(prompt_len, freq, k_cache, v_cache, x_steps, w_norm.reshape(1, model_dim), w_q, w_k, w_v, w_o)
        k_out, v_out, y_out = pl.pallas_call(
            write_kernel,
            out_shape=(cache, cache, jax.ShapeDtypeStruct((n_steps * num_rows, model_dim), BF16)),
            in_specs=[vmem, vmem, vmem],
            out_specs=(any_space, any_space, any_space),
            scratch_shapes=[dma((3,))],
            name="write_out",
        )(k_buf, v_buf, y_buf)
        return y_out.reshape(n_steps, num_rows, model_dim), k_out[:, None], v_out[:, None]

    cache_spec = P("dp", None, "tp", None)
    col_spec = P(None, "tp")
    out_cache_spec = P("dp", "tp", None, None)
    return jax.shard_map(local_block, mesh=mesh, in_specs=(cache_spec, cache_spec, P("dp"), P(None, "dp", None), P(None), col_spec, col_spec, col_spec, P("tp", None)), out_specs=(P(None, "dp", None), out_cache_spec, out_cache_spec), check_vma=False)
```

```python
import functools

import jax
import jax.numpy as jnp
from jax import lax
from jax.experimental import pallas as pl
from jax.experimental.pallas import tpu as pltpu
from jax.sharding import PartitionSpec as P

ROPE_BASE = 10000.0
NORM_EPS = 1e-6
CORES = 2
GROUP_ROWS = 2
BANDS = 2
CUTS = 2
X_STEPS = 8
MESH = pl.DeviceIdType.MESH
BF16 = jnp.bfloat16
F32 = jnp.float32


def main_kernel(n_tp, n_dp, plen_in, freq, gain, k_in, v_in, x_in, w_q, w_k, w_v, w_o, k_buf, v_buf, y_buf,
                plen, wq_v, wk_v, wv_v, x_blk, qkv, q_s, k_n, v_n, o_sr, o_snd, o_all, w_all, x_res,
                in_sem, x_sem, send_sem, recv_sem, w_send, w_recv, dp_send, dp_recv, p_send, p_recv,
                o_send, o_recv, d_send, d_recv):
    num_rows, out_len, head_dim = k_buf.shape
    n_steps, _, model_dim = x_in.shape
    slots = k_in.shape[2]
    seq_len = slots * n_tp
    chips = n_tp // CORES
    far = chips // 2
    half_steps = n_steps // CORES
    band = num_rows // BANDS
    band_rows = half_steps * band
    piece_steps = half_steps // CUTS
    piece = piece_steps * band
    wide = CORES * head_dim
    n_groups = num_rows // GROUP_ROWS
    share = model_dim // n_dp

    dp = lax.axis_index("dp")
    me = lax.axis_index("tp")
    chip = me // CORES
    core = lax.rem(me, CORES)
    other = 1 - core

    def chip_at(offset):
        return lax.rem(chip + offset + chips, chips)

    def device(chip_index, core_index):
        return (dp, chip_index * CORES + core_index)

    def sibling(offset):
        return (lax.rem(dp + offset, n_dp), me)

    partner = device(chip, other)
    offsets = [0] + [s * d for d in range(1, far) for s in (1, -1)] + [far]
    my_lanes = pl.ds(pl.multiple_of(core * head_dim, head_dim), head_dim)

    barrier = pltpu.get_barrier_semaphore()
    for off in offsets:
        for c in range(CORES):
            if (off, c) != (0, 0):
                pl.semaphore_signal(barrier, inc=1, device_id=device(chip_at(off), lax.rem(core + c, CORES)), device_id_type=MESH)
    for off in range(1, n_dp):
        pl.semaphore_signal(barrier, inc=1, device_id=sibling(off), device_id_type=MESH)

    my_share = pl.ds(pl.multiple_of(dp * share, share), share)
    loads = [
        pltpu.make_async_copy(plen_in, plen, in_sem.at[0]),
        pltpu.make_async_copy(w_q, wq_v, in_sem.at[1]),
        pltpu.make_async_copy(w_k, wk_v, in_sem.at[2]),
        pltpu.make_async_copy(w_v, wv_v, in_sem.at[3]),
        pltpu.make_async_copy(w_o.at[:, my_share], w_all.at[chip, my_lanes, my_share], in_sem.at[4]),
        pltpu.make_async_copy(x_in.at[pl.ds(core * half_steps, half_steps)], x_res, in_sem.at[5]),
    ]
    for load in loads:
        load.start()

    def x_load(i, slot):
        return pltpu.make_async_copy(x_in.at[pl.ds(i * X_STEPS, X_STEPS)], x_blk.at[slot], x_sem.at[slot])

    x_load(0, 0).start()

    with jax.named_scope("barrier"):
        pl.semaphore_wait(barrier, n_tp - 1 + n_dp - 1)

    def hops(way, j):
        return far if (way + j) % 2 == 0 else far - 1

    def ring_copy(at, sems, way, hop, j, first=None):
        step = 1 if way == 0 else -1
        view = at(chip_at(-step * (hop - 1)), j)
        return pltpu.make_async_remote_copy(
            src_ref=view if first is None else first, dst_ref=view,
            send_sem=sems[0].at[way, hop - 1, j], recv_sem=sems[1].at[way, hop - 1, j],
            device_id=device(chip_at(step), core), device_id_type=MESH)

    def ring_start(at, sems, hop, pieces):
        for j in pieces:
            for way in range(2):
                if hop <= hops(way, j):
                    ring_copy(at, sems, way, hop, j).start()

    def ring_turn(at, sems, hop, pieces):
        for j in pieces:
            for way in range(2):
                if hop <= hops(way, j):
                    ring_copy(at, sems, way, hop, j).wait_recv()
                    if hop < hops(way, j):
                        ring_copy(at, sems, way, hop + 1, j).start()

    def ring_drain(at, sems, pieces):
        for hop in range(1, far + 1):
            for j in pieces:
                for way in range(2):
                    if hop <= hops(way, j):
                        ring_copy(at, sems, way, hop, j).wait_send()

    w_half = head_dim // 2
    w_sems = (w_send, w_recv)

    def w_at(c, j):
        return w_all.at[c, pl.ds(pl.multiple_of(core * head_dim, head_dim) + j * w_half, w_half), my_share]

    for j in range(2):
        for way in range(2):
            ring_copy(w_at, w_sems, way, 1, j, w_o.at[pl.ds(j * w_half, w_half), my_share]).start()

    my_slots = pl.ds(pl.multiple_of(me * slots, slots), slots)

    def send_group(i, _):
        rows = pl.ds(i * GROUP_ROWS, GROUP_ROWS)
        for which, (src, dst) in enumerate(((k_in, k_buf), (v_in, v_buf))):
            pltpu.make_async_copy(src.at[rows, me], dst.at[rows, my_slots], recv_sem.at[which, i]).start()
            for off in reversed(offsets):
                for c in range(CORES):
                    if (off, c) != (0, 0):
                        to_core = lax.rem(core + c, CORES)
                        to_chip = chip_at(off)
                        pltpu.make_async_remote_copy(
                            src_ref=src.at[rows, to_chip * CORES + to_core],
                            dst_ref=dst.at[rows, my_slots],
                            send_sem=send_sem.at[which, i],
                            recv_sem=recv_sem.at[which, i],
                            device_id=device(to_chip, to_core),
                            device_id_type=MESH,
                        ).start()
        return 0

    send_group(0, 0)

    for load in loads[:4]:
        load.wait()
    n_blocks = n_steps // X_STEPS
    blk_rows = X_STEPS * num_rows

    def project(i, _):
        slot = lax.rem(i, 2)

        @pl.when(i + 1 < n_blocks)
        def _():
            x_load(i + 1, 1 - slot).start()

        x_load(i, slot).wait()
        x = x_blk[slot].reshape(blk_rows, model_dim).astype(F32)
        inv = lax.rsqrt(jnp.mean(x * x, axis=-1, keepdims=True) + NORM_EPS)
        normed = (x * inv * gain[...]).astype(BF16)
        out = pl.ds(pl.multiple_of(i * blk_rows, blk_rows), blk_rows)
        for j, w in enumerate((wq_v, wk_v, wv_v)):
            qkv[j, out, :] = jnp.dot(normed, w[...], preferred_element_type=F32).astype(BF16).astype(F32)
        return 0

    with jax.named_scope("project"):
        lax.fori_loop(0, n_blocks, project, 0)

    with jax.named_scope("w_hop1"):
        ring_turn(w_at, w_sems, 1, range(2))
    send_group(1, 0)

    def rope_row(b, _):
        step_id = lax.broadcasted_iota(jnp.int32, (n_steps, head_dim), 0)
        angle = (step_id + plen[b]).astype(F32) * freq[...]
        lane = lax.broadcasted_iota(jnp.int32, (n_steps, head_dim), 1)
        cos_part = jnp.cos(angle)
        sin_part = jnp.where(lane < head_dim // 2, -1.0, 1.0) * jnp.sin(angle)
        row = pl.ds(b, n_steps, stride=num_rows)

        def rotate(u):
            return u * cos_part + pltpu.roll(u, head_dim // 2, 1) * sin_part

        q_s[b] = (rotate(qkv[0, row, :]) * head_dim ** -0.5).astype(BF16)
        k_n[b] = rotate(qkv[1, row, :]).astype(BF16)
        v_n[b] = qkv[2, row, :].astype(BF16)
        for buf in (k_buf, v_buf):
            buf[b, seq_len:, :] = jnp.zeros((out_len - seq_len, head_dim), BF16)
        return 0

    with jax.named_scope("rope"):
        lax.fori_loop(0, num_rows, rope_row, 0)

    for hop in range(2, far):
        with jax.named_scope(f"w_hop{hop}"):
            ring_turn(w_at, w_sems, hop, range(2))
        send_group(hop, 0)
    with jax.named_scope(f"w_hop{far}"):
        ring_turn(w_at, w_sems, far, range(2))
    loads[4].wait()

    def to_sibling(off):
        view = w_all.at[:, my_lanes, my_share]
        return pltpu.make_async_remote_copy(
            src_ref=view, dst_ref=view, send_sem=dp_send.at[off - 1], recv_sem=dp_recv.at[off - 1],
            device_id=sibling(off), device_id_type=MESH)

    for off in range(1, n_dp):
        to_sibling(off).start()
    lax.fori_loop(far, n_groups, send_group, 0)

    w_swap = pltpu.make_async_remote_copy(
        src_ref=w_all.at[:, my_lanes], dst_ref=w_all.at[:, my_lanes], send_sem=p_send.at[BANDS], recv_sem=p_recv.at[BANDS],
        device_id=partner, device_id_type=MESH)

    def attend_row(b):
        start = plen[b]
        slot_id = lax.broadcasted_iota(jnp.int32, (out_len, n_steps), 0)
        step_id = lax.broadcasted_iota(jnp.int32, (out_len, n_steps), 1)
        pick = jnp.where(slot_id - step_id == start, 1.0, 0.0).astype(BF16)
        at = lax.broadcasted_iota(jnp.int32, (out_len, head_dim), 0) - start
        is_new = jnp.logical_and(at >= 0, at < n_steps)
        for buf, new in ((k_buf, k_n), (v_buf, v_n)):
            placed = jnp.dot(pick, new[b], preferred_element_type=F32)
            buf[b] = jnp.where(is_new, placed, buf[b].astype(F32)).astype(BF16)
        s = lax.dot_general(q_s[b], k_buf[b], (((1,), (1,)), ((), ())), preferred_element_type=F32)
        s_slot = lax.broadcasted_iota(jnp.int32, (n_steps, out_len), 1)
        s_step = lax.broadcasted_iota(jnp.int32, (n_steps, out_len), 0)
        s = jnp.where(s_slot - s_step <= start, s, -jnp.inf)
        e = jnp.exp(s - jnp.max(s, axis=-1, keepdims=True))
        a = (e / jnp.sum(e, axis=-1, keepdims=True)).astype(BF16)
        o = jnp.dot(a, v_buf[b], preferred_element_type=F32)
        o_sr[b // band, pl.ds(lax.rem(b, band), n_steps, stride=band), :] = o.astype(BF16).astype(F32)

    mine = pl.ds(pl.multiple_of(core * band_rows, band_rows), band_rows)
    theirs = pl.ds(pl.multiple_of(other * band_rows, band_rows), band_rows)
    o_sems = (o_send, o_recv)

    def swap(h):
        return pltpu.make_async_remote_copy(
            src_ref=o_snd.at[h], dst_ref=o_all.at[chip, pl.ds(h * band_rows, band_rows), my_lanes],
            send_sem=p_send.at[h], recv_sem=p_recv.at[h], device_id=partner, device_id_type=MESH)

    def swap_start(h):
        o_snd[h] = o_sr[h, theirs, :].astype(BF16)
        swap(h).start()
        o_all[chip, h * band_rows:(h + 1) * band_rows, my_lanes] = o_sr[h, mine, :].astype(BF16)

    def o_at(c, j):
        return o_all.at[c, pl.ds(j * piece, piece)]

    def band_pieces(h):
        return range(h * CUTS, (h + 1) * CUTS)

    def attend_group(i, _):
        rows = pl.ds(i * GROUP_ROWS, GROUP_ROWS)
        with jax.named_scope("wait_group"):
            for which, buf in enumerate((k_buf, v_buf)):
                got = buf.at[rows, pl.ds(0, seq_len)]
                pltpu.make_async_copy(got, got, recv_sem.at[which, i]).wait()
        with jax.named_scope("attend_group"):
            for r in range(GROUP_ROWS):
                attend_row(i * GROUP_ROWS + r)

        @pl.when(i == n_groups // 2 - 1)
        def _():
            swap_start(0)

        @pl.when(i == n_groups // 2)
        def _():
            swap(0).wait_recv()
            ring_start(o_at, o_sems, 1, band_pieces(0))

        @pl.when(i == n_groups - 3)
        def _():
            for off in range(1, n_dp):
                to_sibling(off).wait_recv()
            w_swap.start()

        return 0

    lax.fori_loop(0, n_groups, attend_group, 0)

    def y_at(of_core, j):
        first = pl.multiple_of(of_core * half_steps, half_steps) + (j % CUTS) * piece_steps
        return (pl.ds(first, piece_steps), pl.ds(j // CUTS * band, band))

    def hand_on(of_core, j):
        view = y_buf.at[y_at(of_core, j)]
        return pltpu.make_async_remote_copy(
            src_ref=view, dst_ref=view, send_sem=d_send.at[j], recv_sem=d_recv.at[j],
            device_id=partner, device_id_type=MESH)

    def y_piece(j):
        steps, rows = y_at(core, j)
        local = pl.ds((j % CUTS) * piece_steps, piece_steps)

        def columns(n, _):
            cols = pl.ds(pl.multiple_of(n * wide, wide), wide)
            total = jnp.dot(o_all[0, j * piece:(j + 1) * piece, :], w_all[0, :, cols], preferred_element_type=F32)
            for c in range(1, chips):
                total += jnp.dot(o_all[c, j * piece:(j + 1) * piece, :], w_all[c, :, cols], preferred_element_type=F32)
            x = x_res[local, rows, cols].astype(F32)
            y_buf[steps, rows, cols] = (x + total.reshape(piece_steps, band, wide)).astype(BF16)
            return 0

        with jax.named_scope("y_piece"):
            lax.fori_loop(0, model_dim // wide, columns, 0)
            hand_on(core, j).start()

    with jax.named_scope("swap1"):
        swap_start(1)
    with jax.named_scope("o_b0_hop1"):
        ring_turn(o_at, o_sems, 1, band_pieces(0))
    with jax.named_scope("o_b1_start"):
        swap(1).wait_recv()
        ring_start(o_at, o_sems, 1, band_pieces(1))
    loads[5].wait()
    w_swap.wait_recv()
    for hop in range(2, far + 1):
        with jax.named_scope(f"o_b0_hop{hop}"):
            ring_turn(o_at, o_sems, hop, band_pieces(0))
        with jax.named_scope(f"o_b1_hop{hop - 1}"):
            ring_turn(o_at, o_sems, hop - 1, band_pieces(1))
    for j in band_pieces(0):
        y_piece(j)
    for j in band_pieces(1):
        with jax.named_scope(f"o_b1_hop{far}"):
            ring_turn(o_at, o_sems, far, [j])
        y_piece(j)

    with jax.named_scope("drain"):
        for i in range(n_groups):
            rows = pl.ds(i * GROUP_ROWS, GROUP_ROWS)
            for which, buf in enumerate((k_buf, v_buf)):
                sent = buf.at[rows, pl.ds(0, seq_len - slots)]
                pltpu.make_async_copy(sent, sent, send_sem.at[which, i]).wait()
        ring_drain(w_at, w_sems, range(2))
        ring_drain(o_at, o_sems, range(BANDS * CUTS))
        for off in range(1, n_dp):
            to_sibling(off).wait_send()
        w_swap.wait_send()
        for h in range(BANDS):
            swap(h).wait_send()
        for j in range(BANDS * CUTS):
            hand_on(core, j).wait_send()
            hand_on(other, j).wait_recv()


def write_kernel(k_buf, v_buf, y_buf, k_out, v_out, y_out, sem):
    parts = sem.shape[1]
    copies = []
    for a, (src, dst) in enumerate(((k_buf, k_out), (v_buf, v_out), (y_buf, y_out))):
        size = src.shape[0] // parts
        for i in range(parts):
            copies.append(pltpu.make_async_copy(src.at[pl.ds(i * size, size)], dst.at[pl.ds(i * size, size)], sem.at[a, i]))
    for copy in copies:
        copy.start()
    for copy in copies:
        copy.wait()


def solution(mesh):
    n_tp = mesh.shape["tp"]
    n_dp = mesh.shape["dp"]

    def local_block(k_cache, v_cache, prompt_len, x_steps, w_norm, w_q, w_k, w_v, w_o):
        num_rows, _, slots, head_dim = k_cache.shape
        n_steps, _, model_dim = x_steps.shape
        out_len = slots * n_tp + n_steps
        chips = n_tp // CORES
        far = chips // 2
        half_steps = n_steps // CORES
        half_rows = half_steps * num_rows
        wide = CORES * head_dim
        n_groups = num_rows // GROUP_ROWS
        pieces = BANDS * CUTS
        lanes = jnp.arange(head_dim, dtype=jnp.int32) % (head_dim // 2)
        freq = (ROPE_BASE ** (-2.0 * lanes.astype(F32) / head_dim)).reshape(1, head_dim)
        gain = (1.0 + w_norm.astype(F32)).reshape(1, model_dim)
        dma = pltpu.SemaphoreType.DMA
        in_hbm = functools.partial(pltpu.with_memory_space_constraint, memory_space=pltpu.HBM)

        def in_vmem(shape):
            return pltpu.VMEM(shape.shape, shape.dtype)

        hbm = pl.BlockSpec(memory_space=pltpu.HBM)
        vmem = pl.BlockSpec(memory_space=pltpu.VMEM)
        cache = jax.ShapeDtypeStruct((num_rows, out_len, head_dim), BF16)
        y_shape = jax.ShapeDtypeStruct(x_steps.shape, BF16)
        k_buf, v_buf, y_buf = pl.pallas_call(
            functools.partial(main_kernel, n_tp, n_dp),
            out_shape=(in_vmem(cache), in_vmem(cache), in_vmem(y_shape)),
            in_specs=[hbm, vmem, vmem] + [hbm] * 7,
            out_specs=(vmem, vmem, vmem),
            scratch_shapes=[
                pltpu.SMEM(prompt_len.shape, jnp.int32),
                pltpu.VMEM((model_dim, head_dim), BF16),
                pltpu.VMEM((model_dim, head_dim), BF16),
                pltpu.VMEM((model_dim, head_dim), BF16),
                pltpu.VMEM((2, X_STEPS, num_rows, model_dim), BF16),
                pltpu.VMEM((3, n_steps * num_rows, head_dim), F32),
                pltpu.VMEM((num_rows, n_steps, head_dim), BF16),
                pltpu.VMEM((num_rows, n_steps, head_dim), BF16),
                pltpu.VMEM((num_rows, n_steps, head_dim), BF16),
                pltpu.VMEM((BANDS, n_steps * num_rows // BANDS, head_dim), F32),
                pltpu.VMEM((BANDS, half_rows // BANDS, head_dim), BF16),
                pltpu.VMEM((chips, half_rows, wide), BF16),
                pltpu.VMEM((chips, wide, model_dim), BF16),
                pltpu.VMEM((half_steps, num_rows, model_dim), BF16),
                dma((6,)), dma((2,)),
                dma((2, n_groups)), dma((2, n_groups)),
                dma((2, far, 2)), dma((2, far, 2)),
                dma((n_dp,)), dma((n_dp,)),
                dma((BANDS + 1,)), dma((BANDS + 1,)),
                dma((2, far, pieces)), dma((2, far, pieces)),
                dma((pieces,)), dma((pieces,)),
            ],
            compiler_params=pltpu.CompilerParams(collective_id=0, has_side_effects=True, vmem_limit_bytes=28 * 2**20),
            name="decode_block",
        )(in_hbm(prompt_len), freq, gain, *map(in_hbm, (k_cache, v_cache, x_steps, w_q, w_k, w_v, w_o)))
        k_out, v_out, y_out = pl.pallas_call(
            write_kernel,
            out_shape=(cache, cache, y_shape),
            in_specs=[vmem, vmem, vmem],
            out_specs=(hbm, hbm, hbm),
            scratch_shapes=[dma((3, 8))],
            compiler_params=pltpu.CompilerParams(vmem_limit_bytes=4 * 2**20),
            name="write_out",
        )(k_buf, v_buf, y_buf)
        return y_out, k_out[:, None], v_out[:, None]

    cache_spec = P("dp", None, "tp", None)
    col_spec = P(None, "tp")
    out_cache_spec = P("dp", "tp", None, None)
    return jax.shard_map(local_block, mesh=mesh, in_specs=(cache_spec, cache_spec, P("dp"), P(None, "dp", None), P(None), col_spec, col_spec, col_spec, P("tp", None)), out_specs=(P(None, "dp", None), out_cache_spec, out_cache_spec), check_vma=False)
```

```python
import functools

import jax
import jax.numpy as jnp
from jax import lax
from jax.experimental import pallas as pl
from jax.experimental.pallas import tpu as pltpu
from jax.sharding import PartitionSpec as P

ROPE_BASE = 10000.0
NORM_EPS = 1e-6
CORES = 2
GROUP_ROWS = 2
BANDS = 2
CUTS = 2
X_STEPS = 8
MESH = pl.DeviceIdType.MESH
BF16 = jnp.bfloat16
F32 = jnp.float32


def main_kernel(n_tp, n_dp, plen_in, freq, gain, k_in, v_in, x_in, w_q, w_k, w_v, w_o, k_buf, v_buf, y_buf,
                plen, wq_v, wk_v, wv_v, x_blk, qkv, q_s, k_n, v_n, o_sr, o_snd, o_all, w_all, x_res, y_acc,
                in_sem, x_sem, send_sem, recv_sem, w_send, w_recv, dp_send, dp_recv, p_send, p_recv,
                o_send, o_recv, d_send, d_recv):
    num_rows, out_len, head_dim = k_buf.shape
    n_steps, _, model_dim = x_in.shape
    slots = k_in.shape[2]
    seq_len = slots * n_tp
    chips = n_tp // CORES
    far = chips // 2
    half_steps = n_steps // CORES
    band = num_rows // BANDS
    band_rows = half_steps * band
    piece_steps = half_steps // CUTS
    piece = piece_steps * band
    wide = CORES * head_dim
    n_groups = num_rows // GROUP_ROWS
    share = model_dim // n_dp
    quarter = y_acc.shape[1] // d_send.shape[1]

    dp = lax.axis_index("dp")
    me = lax.axis_index("tp")
    chip = me // CORES
    core = lax.rem(me, CORES)
    other = 1 - core

    def chip_at(offset):
        return lax.rem(chip + offset + chips, chips)

    def device(chip_index, core_index):
        return (dp, chip_index * CORES + core_index)

    def sibling(offset):
        return (lax.rem(dp + offset, n_dp), me)

    partner = device(chip, other)
    offsets = [0] + [s * d for d in range(1, far) for s in (1, -1)] + [far]
    my_lanes = pl.ds(pl.multiple_of(core * head_dim, head_dim), head_dim)

    barrier = pltpu.get_barrier_semaphore()
    for off in offsets:
        for c in range(CORES):
            if (off, c) != (0, 0):
                pl.semaphore_signal(barrier, inc=1, device_id=device(chip_at(off), lax.rem(core + c, CORES)), device_id_type=MESH)
    for off in range(1, n_dp):
        pl.semaphore_signal(barrier, inc=1, device_id=sibling(off), device_id_type=MESH)

    my_share = pl.ds(pl.multiple_of(dp * share, share), share)
    loads = [
        pltpu.make_async_copy(plen_in, plen, in_sem.at[0]),
        pltpu.make_async_copy(w_q, wq_v, in_sem.at[1]),
        pltpu.make_async_copy(w_k, wk_v, in_sem.at[2]),
        pltpu.make_async_copy(w_v, wv_v, in_sem.at[3]),
        pltpu.make_async_copy(w_o.at[:, my_share], w_all.at[chip, my_lanes, my_share], in_sem.at[4]),
        pltpu.make_async_copy(x_in.at[pl.ds(core * half_steps, half_steps)], x_res, in_sem.at[5]),
    ]
    for load in loads:
        load.start()

    def x_load(i, slot):
        return pltpu.make_async_copy(x_in.at[pl.ds(i * X_STEPS, X_STEPS)], x_blk.at[slot], x_sem.at[slot])

    x_load(0, 0).start()

    with jax.named_scope("barrier"):
        pl.semaphore_wait(barrier, n_tp - 1 + n_dp - 1)

    def hops(way, j):
        return far if (way + j) % 2 == 0 else far - 1

    def ring_copy(at, sems, way, hop, j, first=None):
        step = 1 if way == 0 else -1
        view = at(chip_at(-step * (hop - 1)), j)
        return pltpu.make_async_remote_copy(
            src_ref=view if first is None else first, dst_ref=view,
            send_sem=sems[0].at[way, hop - 1, j], recv_sem=sems[1].at[way, hop - 1, j],
            device_id=device(chip_at(step), core), device_id_type=MESH)

    def ring_start(at, sems, hop, pieces):
        for j in pieces:
            for way in range(2):
                if hop <= hops(way, j):
                    ring_copy(at, sems, way, hop, j).start()

    def ring_turn(at, sems, hop, pieces):
        for j in pieces:
            for way in range(2):
                if hop <= hops(way, j):
                    ring_copy(at, sems, way, hop, j).wait_recv()
                    if hop < hops(way, j):
                        ring_copy(at, sems, way, hop + 1, j).start()

    def ring_drain(at, sems, pieces):
        for hop in range(1, far + 1):
            for j in pieces:
                for way in range(2):
                    if hop <= hops(way, j):
                        ring_copy(at, sems, way, hop, j).wait_send()

    w_half = head_dim // 2
    w_sems = (w_send, w_recv)

    def w_at(c, j):
        return w_all.at[c, pl.ds(pl.multiple_of(core * head_dim, head_dim) + j * w_half, w_half), my_share]

    for j in range(2):
        for way in range(2):
            ring_copy(w_at, w_sems, way, 1, j, w_o.at[pl.ds(j * w_half, w_half), my_share]).start()

    my_slots = pl.ds(pl.multiple_of(me * slots, slots), slots)

    def send_group(i, _):
        rows = pl.ds(i * GROUP_ROWS, GROUP_ROWS)
        for which, (src, dst) in enumerate(((k_in, k_buf), (v_in, v_buf))):
            pltpu.make_async_copy(src.at[rows, me], dst.at[rows, my_slots], recv_sem.at[which, i]).start()
            for off in reversed(offsets):
                for c in range(CORES):
                    if (off, c) != (0, 0):
                        to_core = lax.rem(core + c, CORES)
                        to_chip = chip_at(off)
                        pltpu.make_async_remote_copy(
                            src_ref=src.at[rows, to_chip * CORES + to_core],
                            dst_ref=dst.at[rows, my_slots],
                            send_sem=send_sem.at[which, i],
                            recv_sem=recv_sem.at[which, i],
                            device_id=device(to_chip, to_core),
                            device_id_type=MESH,
                        ).start()
        return 0

    send_group(0, 0)

    for load in loads[:4]:
        load.wait()
    n_blocks = n_steps // X_STEPS
    blk_rows = X_STEPS * num_rows

    def project(i, _):
        slot = lax.rem(i, 2)

        @pl.when(i + 1 < n_blocks)
        def _():
            x_load(i + 1, 1 - slot).start()

        x_load(i, slot).wait()
        x = x_blk[slot].reshape(blk_rows, model_dim).astype(F32)
        inv = lax.rsqrt(jnp.mean(x * x, axis=-1, keepdims=True) + NORM_EPS)
        normed = (x * inv * gain[...]).astype(BF16)
        out = pl.ds(pl.multiple_of(i * blk_rows, blk_rows), blk_rows)
        for j, w in enumerate((wq_v, wk_v, wv_v)):
            qkv[j, out, :] = jnp.dot(normed, w[...], preferred_element_type=F32).astype(BF16).astype(F32)
        return 0

    with jax.named_scope("project"):
        lax.fori_loop(0, n_blocks, project, 0)

    with jax.named_scope("w_hop1"):
        ring_turn(w_at, w_sems, 1, range(2))
    send_group(1, 0)

    def rope_row(b, _):
        step_id = lax.broadcasted_iota(jnp.int32, (n_steps, head_dim), 0)
        angle = (step_id + plen[b]).astype(F32) * freq[...]
        lane = lax.broadcasted_iota(jnp.int32, (n_steps, head_dim), 1)
        cos_part = jnp.cos(angle)
        sin_part = jnp.where(lane < head_dim // 2, -1.0, 1.0) * jnp.sin(angle)
        row = pl.ds(b, n_steps, stride=num_rows)

        def rotate(u):
            return u * cos_part + pltpu.roll(u, head_dim // 2, 1) * sin_part

        q_s[b] = (rotate(qkv[0, row, :]) * head_dim ** -0.5).astype(BF16)
        k_n[b] = rotate(qkv[1, row, :]).astype(BF16)
        v_n[b] = qkv[2, row, :].astype(BF16)
        for buf in (k_buf, v_buf):
            buf[b, seq_len:, :] = jnp.zeros((out_len - seq_len, head_dim), BF16)
        return 0

    with jax.named_scope("rope"):
        lax.fori_loop(0, num_rows, rope_row, 0)

    for hop in range(2, far):
        with jax.named_scope(f"w_hop{hop}"):
            ring_turn(w_at, w_sems, hop, range(2))
        send_group(hop, 0)
    with jax.named_scope(f"w_hop{far}"):
        ring_turn(w_at, w_sems, far, range(2))
    loads[4].wait()

    def to_sibling(off):
        view = w_all.at[:, my_lanes, my_share]
        return pltpu.make_async_remote_copy(
            src_ref=view, dst_ref=view, send_sem=dp_send.at[off - 1], recv_sem=dp_recv.at[off - 1],
            device_id=sibling(off), device_id_type=MESH)

    for off in range(1, n_dp):
        to_sibling(off).start()
    lax.fori_loop(far, n_groups, send_group, 0)

    w_swap = pltpu.make_async_remote_copy(
        src_ref=w_all.at[:, my_lanes], dst_ref=w_all.at[:, my_lanes], send_sem=p_send.at[BANDS], recv_sem=p_recv.at[BANDS],
        device_id=partner, device_id_type=MESH)

    def attend_row(b):
        start = plen[b]
        slot_id = lax.broadcasted_iota(jnp.int32, (out_len, n_steps), 0)
        step_id = lax.broadcasted_iota(jnp.int32, (out_len, n_steps), 1)
        pick = jnp.where(slot_id - step_id == start, 1.0, 0.0).astype(BF16)
        at = lax.broadcasted_iota(jnp.int32, (out_len, head_dim), 0) - start
        is_new = jnp.logical_and(at >= 0, at < n_steps)
        for buf, new in ((k_buf, k_n), (v_buf, v_n)):
            placed = jnp.dot(pick, new[b], preferred_element_type=F32)
            buf[b] = jnp.where(is_new, placed, buf[b].astype(F32)).astype(BF16)
        s = lax.dot_general(q_s[b], k_buf[b], (((1,), (1,)), ((), ())), preferred_element_type=F32)
        s_slot = lax.broadcasted_iota(jnp.int32, (n_steps, out_len), 1)
        s_step = lax.broadcasted_iota(jnp.int32, (n_steps, out_len), 0)
        s = jnp.where(s_slot - s_step <= start, s, -jnp.inf)
        e = jnp.exp(s - jnp.max(s, axis=-1, keepdims=True))
        a = (e / jnp.sum(e, axis=-1, keepdims=True)).astype(BF16)
        o = jnp.dot(a, v_buf[b], preferred_element_type=F32)
        o_sr[b // band, pl.ds(lax.rem(b, band), n_steps, stride=band), :] = o.astype(BF16).astype(F32)

    mine = pl.ds(pl.multiple_of(core * band_rows, band_rows), band_rows)
    theirs = pl.ds(pl.multiple_of(other * band_rows, band_rows), band_rows)
    o_sems = (o_send, o_recv)

    def swap(h):
        return pltpu.make_async_remote_copy(
            src_ref=o_snd.at[h], dst_ref=o_all.at[chip, pl.ds(h * band_rows, band_rows), my_lanes],
            send_sem=p_send.at[h], recv_sem=p_recv.at[h], device_id=partner, device_id_type=MESH)

    def swap_start(h):
        o_snd[h] = o_sr[h, theirs, :].astype(BF16)
        swap(h).start()
        o_all[chip, h * band_rows:(h + 1) * band_rows, my_lanes] = o_sr[h, mine, :].astype(BF16)

    def o_at(c, j):
        return o_all.at[c, pl.ds(j * piece, piece)]

    def band_pieces(h):
        return range(h * CUTS, (h + 1) * CUTS)

    def attend_group(i, _):
        rows = pl.ds(i * GROUP_ROWS, GROUP_ROWS)
        with jax.named_scope("wait_group"):
            for which, buf in enumerate((k_buf, v_buf)):
                got = buf.at[rows, pl.ds(0, seq_len)]
                pltpu.make_async_copy(got, got, recv_sem.at[which, i]).wait()
        with jax.named_scope("attend_group"):
            for r in range(GROUP_ROWS):
                attend_row(i * GROUP_ROWS + r)

        @pl.when(i == n_groups // 2 - 1)
        def _():
            swap_start(0)

        @pl.when(i == n_groups // 2)
        def _():
            swap(0).wait_recv()
            ring_start(o_at, o_sems, 1, band_pieces(0))

        @pl.when(i == n_groups - 3)
        def _():
            for off in range(1, n_dp):
                to_sibling(off).wait_recv()
            w_swap.start()

        return 0

    lax.fori_loop(0, n_groups, attend_group, 0)

    def y_view(of_core, h, cols):
        return y_buf.at[pl.ds(pl.multiple_of(of_core * half_steps, half_steps), half_steps), pl.ds(h * band, band), cols]

    def hand_on(of_core, h, q):
        view = y_view(of_core, h, pl.ds(q * quarter, quarter))
        return pltpu.make_async_remote_copy(
            src_ref=view, dst_ref=view, send_sem=d_send.at[h, q], recv_sem=d_recv.at[h, q],
            device_id=partner, device_id_type=MESH)

    def y_add(h, froms, first=False, last=False):
        rows = slice(h * band_rows, (h + 1) * band_rows)
        for n in range(model_dim // wide):
            cols = slice(n * wide, (n + 1) * wide)
            total = None
            for off in froms:
                c = chip_at(off)
                part = jnp.dot(o_all[c, rows, :], w_all[c, :, cols], preferred_element_type=F32)
                total = part if total is None else total + part
            if first:
                total += x_res[:, h * band:(h + 1) * band, cols].astype(F32).reshape(band_rows, wide)
            else:
                total += y_acc[:, cols]
            if last:
                y_view(core, h, pl.ds(n * wide, wide))[...] = total.reshape(half_steps, band, wide).astype(BF16)
                if (n + 1) * wide % quarter == 0:
                    hand_on(core, h, n * wide // quarter).start()
            else:
                y_acc[:, cols] = total

    def turn(h, hop):
        with jax.named_scope(f"o_b{h}_hop{hop}"):
            ring_turn(o_at, o_sems, hop, band_pieces(h))

    def add(h, froms, **kwargs):
        with jax.named_scope(f"y_b{h}"):
            y_add(h, froms, **kwargs)

    near = [s * d for d in range(1, far - 1) for s in (1, -1)]
    edge = [far - 1, 1 - far]
    swap_start(1)
    turn(0, 1)
    with jax.named_scope("o_b1_start"):
        swap(1).wait_recv()
        ring_start(o_at, o_sems, 1, band_pieces(1))
    loads[5].wait()
    w_swap.wait_recv()
    for hop in range(2, far + 1):
        turn(0, hop)
        if hop == far - 2:
            add(0, [0] + near, first=True)
        if hop == far - 1:
            add(0, edge)
        if hop == far:
            add(0, [far], last=True)
        turn(1, hop - 1)
        if hop - 1 == far - 1:
            add(1, [0] + near + edge, first=True)
    turn(1, far)
    add(1, [far], last=True)

    with jax.named_scope("drain"):
        for i in range(n_groups):
            rows = pl.ds(i * GROUP_ROWS, GROUP_ROWS)
            for which, buf in enumerate((k_buf, v_buf)):
                sent = buf.at[rows, pl.ds(0, seq_len - slots)]
                pltpu.make_async_copy(sent, sent, send_sem.at[which, i]).wait()
        ring_drain(w_at, w_sems, range(2))
        ring_drain(o_at, o_sems, range(BANDS * CUTS))
        for off in range(1, n_dp):
            to_sibling(off).wait_send()
        w_swap.wait_send()
        for h in range(BANDS):
            swap(h).wait_send()
        for h in range(BANDS):
            for q in range(model_dim // quarter):
                hand_on(core, h, q).wait_send()
                hand_on(other, h, q).wait_recv()


def write_kernel(k_buf, v_buf, y_buf, k_out, v_out, y_out, sem):
    parts = sem.shape[1]
    copies = []
    for a, (src, dst) in enumerate(((k_buf, k_out), (v_buf, v_out), (y_buf, y_out))):
        size = src.shape[0] // parts
        for i in range(parts):
            copies.append(pltpu.make_async_copy(src.at[pl.ds(i * size, size)], dst.at[pl.ds(i * size, size)], sem.at[a, i]))
    for copy in copies:
        copy.start()
    for copy in copies:
        copy.wait()


def solution(mesh):
    n_tp = mesh.shape["tp"]
    n_dp = mesh.shape["dp"]

    def local_block(k_cache, v_cache, prompt_len, x_steps, w_norm, w_q, w_k, w_v, w_o):
        num_rows, _, slots, head_dim = k_cache.shape
        n_steps, _, model_dim = x_steps.shape
        out_len = slots * n_tp + n_steps
        chips = n_tp // CORES
        far = chips // 2
        half_steps = n_steps // CORES
        half_rows = half_steps * num_rows
        wide = CORES * head_dim
        n_groups = num_rows // GROUP_ROWS
        pieces = BANDS * CUTS
        lanes = jnp.arange(head_dim, dtype=jnp.int32) % (head_dim // 2)
        freq = (ROPE_BASE ** (-2.0 * lanes.astype(F32) / head_dim)).reshape(1, head_dim)
        gain = (1.0 + w_norm.astype(F32)).reshape(1, model_dim)
        dma = pltpu.SemaphoreType.DMA
        in_hbm = functools.partial(pltpu.with_memory_space_constraint, memory_space=pltpu.HBM)

        def in_vmem(shape):
            return pltpu.VMEM(shape.shape, shape.dtype)

        hbm = pl.BlockSpec(memory_space=pltpu.HBM)
        vmem = pl.BlockSpec(memory_space=pltpu.VMEM)
        cache = jax.ShapeDtypeStruct((num_rows, out_len, head_dim), BF16)
        y_shape = jax.ShapeDtypeStruct(x_steps.shape, BF16)
        k_buf, v_buf, y_buf = pl.pallas_call(
            functools.partial(main_kernel, n_tp, n_dp),
            out_shape=(in_vmem(cache), in_vmem(cache), in_vmem(y_shape)),
            in_specs=[hbm, vmem, vmem] + [hbm] * 7,
            out_specs=(vmem, vmem, vmem),
            scratch_shapes=[
                pltpu.SMEM(prompt_len.shape, jnp.int32),
                pltpu.VMEM((model_dim, head_dim), BF16),
                pltpu.VMEM((model_dim, head_dim), BF16),
                pltpu.VMEM((model_dim, head_dim), BF16),
                pltpu.VMEM((2, X_STEPS, num_rows, model_dim), BF16),
                pltpu.VMEM((3, n_steps * num_rows, head_dim), F32),
                pltpu.VMEM((num_rows, n_steps, head_dim), BF16),
                pltpu.VMEM((num_rows, n_steps, head_dim), BF16),
                pltpu.VMEM((num_rows, n_steps, head_dim), BF16),
                pltpu.VMEM((BANDS, n_steps * num_rows // BANDS, head_dim), F32),
                pltpu.VMEM((BANDS, half_rows // BANDS, head_dim), BF16),
                pltpu.VMEM((chips, half_rows, wide), BF16),
                pltpu.VMEM((chips, wide, model_dim), BF16),
                pltpu.VMEM((half_steps, num_rows, model_dim), BF16),
                pltpu.VMEM((half_rows // BANDS, model_dim), F32),
                dma((6,)), dma((2,)),
                dma((2, n_groups)), dma((2, n_groups)),
                dma((2, far, 2)), dma((2, far, 2)),
                dma((n_dp,)), dma((n_dp,)),
                dma((BANDS + 1,)), dma((BANDS + 1,)),
                dma((2, far, pieces)), dma((2, far, pieces)),
                dma((BANDS, 4)), dma((BANDS, 4)),
            ],
            compiler_params=pltpu.CompilerParams(collective_id=0, has_side_effects=True, vmem_limit_bytes=28 * 2**20),
            name="decode_block",
        )(in_hbm(prompt_len), freq, gain, *map(in_hbm, (k_cache, v_cache, x_steps, w_q, w_k, w_v, w_o)))
        k_out, v_out, y_out = pl.pallas_call(
            write_kernel,
            out_shape=(cache, cache, y_shape),
            in_specs=[vmem, vmem, vmem],
            out_specs=(hbm, hbm, hbm),
            scratch_shapes=[dma((3, 8))],
            compiler_params=pltpu.CompilerParams(vmem_limit_bytes=4 * 2**20),
            name="write_out",
        )(k_buf, v_buf, y_buf)
        return y_out, k_out[:, None], v_out[:, None]

    cache_spec = P("dp", None, "tp", None)
    col_spec = P(None, "tp")
    out_cache_spec = P("dp", "tp", None, None)
    return jax.shard_map(local_block, mesh=mesh, in_specs=(cache_spec, cache_spec, P("dp"), P(None, "dp", None), P(None), col_spec, col_spec, col_spec, P("tp", None)), out_specs=(P(None, "dp", None), out_cache_spec, out_cache_spec), check_vma=False)
```

```python
import functools

import jax
import jax.numpy as jnp
from jax import lax
from jax.experimental import pallas as pl
from jax.experimental.pallas import tpu as pltpu
from jax.sharding import PartitionSpec as P

ROPE_BASE = 10000.0
NORM_EPS = 1e-6
CORES = 2
GROUP_ROWS = 2
BANDS = 2
CUTS = 2
X_STEPS = 8
MESH = pl.DeviceIdType.MESH
BF16 = jnp.bfloat16
F32 = jnp.float32


def main_kernel(n_tp, n_dp, plen_in, freq, w_norm, k_in, v_in, x_in, w_q, w_k, w_v, w_o, k_buf, v_buf, y_buf,
                plen, norm_v, gain, wq_v, wk_v, wv_v, x_blk, qkv, q_s, k_n, v_n, o_sr, o_snd, o_all, w_all, x_res, y_acc,
                in_sem, x_sem, send_sem, recv_sem, w_send, w_recv, dp_send, dp_recv, p_send, p_recv,
                o_send, o_recv, d_send, d_recv):
    num_rows, out_len, head_dim = k_buf.shape
    n_steps, _, model_dim = x_in.shape
    slots = k_in.shape[2]
    seq_len = slots * n_tp
    chips = n_tp // CORES
    far = chips // 2
    half_steps = n_steps // CORES
    band = num_rows // BANDS
    band_rows = half_steps * band
    piece_steps = half_steps // CUTS
    piece = piece_steps * band
    wide = CORES * head_dim
    n_groups = num_rows // GROUP_ROWS
    share = model_dim // n_dp
    quarter = model_dim // 4

    dp = lax.axis_index("dp")
    me = lax.axis_index("tp")
    chip = me // CORES
    core = lax.rem(me, CORES)
    other = 1 - core

    def chip_at(offset):
        return lax.rem(chip + offset + chips, chips)

    def device(chip_index, core_index):
        return (dp, chip_index * CORES + core_index)

    def sibling(offset):
        return (lax.rem(dp + offset, n_dp), me)

    partner = device(chip, other)
    offsets = [0] + [s * d for d in range(1, far) for s in (1, -1)] + [far]
    my_lanes = pl.ds(pl.multiple_of(core * head_dim, head_dim), head_dim)

    barrier = pltpu.get_barrier_semaphore()
    for off in offsets:
        for c in range(CORES):
            if (off, c) != (0, 0):
                pl.semaphore_signal(barrier, inc=1, device_id=device(chip_at(off), lax.rem(core + c, CORES)), device_id_type=MESH)
    for off in range(1, n_dp):
        pl.semaphore_signal(barrier, inc=1, device_id=sibling(off), device_id_type=MESH)

    my_share = pl.ds(pl.multiple_of(dp * share, share), share)
    loads = [
        pltpu.make_async_copy(plen_in, plen, in_sem.at[0]),
        pltpu.make_async_copy(w_q, wq_v, in_sem.at[1]),
        pltpu.make_async_copy(w_k, wk_v, in_sem.at[2]),
        pltpu.make_async_copy(w_v, wv_v, in_sem.at[3]),
        pltpu.make_async_copy(w_o.at[:, my_share], w_all.at[chip, my_lanes, my_share], in_sem.at[4]),
        pltpu.make_async_copy(x_in.at[pl.ds(core * half_steps, half_steps)], x_res, in_sem.at[5]),
        pltpu.make_async_copy(w_norm, norm_v, in_sem.at[6]),
    ]
    for load in loads:
        load.start()

    def x_load(i, slot):
        return pltpu.make_async_copy(x_in.at[pl.ds(i * X_STEPS, X_STEPS)], x_blk.at[slot], x_sem.at[slot])

    x_load(0, 0).start()

    with jax.named_scope("barrier"):
        pl.semaphore_wait(barrier, n_tp - 1 + n_dp - 1)

    def hops(way, j):
        return far if (way + j) % 2 == 0 else far - 1

    def ring_copy(at, sems, way, hop, j, first=None):
        step = 1 if way == 0 else -1
        view = at(chip_at(-step * (hop - 1)), j)
        return pltpu.make_async_remote_copy(
            src_ref=view if first is None else first, dst_ref=view,
            send_sem=sems[0], recv_sem=sems[1].at[way, hop - 1, j],
            device_id=device(chip_at(step), core), device_id_type=MESH)

    def legs(hop, pieces):
        by_way = [sorted(pieces, key=lambda j, way=way: -hops(way, j)) for way in range(2)]
        return [(way, js[way]) for js in zip(*by_way) for way in range(2) if hop <= hops(way, js[way])]

    def ring_start(at, sems, hop, pieces):
        for way, j in legs(hop, pieces):
            ring_copy(at, sems, way, hop, j).start()

    def ring_turn(at, sems, hop, pieces):
        for way, j in legs(hop, pieces):
            ring_copy(at, sems, way, hop, j).wait_recv()
            if hop < hops(way, j):
                ring_copy(at, sems, way, hop + 1, j).start()

    def wait_bytes(view, sem):
        pltpu.make_async_copy(view, view, sem).wait()

    w_half = head_dim // 2
    w_sems = (w_send, w_recv)

    def w_at(c, j):
        return w_all.at[c, pl.ds(pl.multiple_of(core * head_dim, head_dim) + j * w_half, w_half), my_share]

    for way, j in legs(1, range(2)):
        ring_copy(w_at, w_sems, way, 1, j, w_o.at[pl.ds(j * w_half, w_half), my_share]).start()

    my_slots = pl.ds(pl.multiple_of(me * slots, slots), slots)

    def send_group(i, _):
        rows = pl.ds(i * GROUP_ROWS, GROUP_ROWS)
        for which, (src, dst) in enumerate(((k_in, k_buf), (v_in, v_buf))):
            pltpu.make_async_copy(src.at[rows, me], dst.at[rows, my_slots], recv_sem.at[which, i]).start()
            for off in reversed(offsets):
                for c in range(CORES):
                    if (off, c) != (0, 0):
                        to_core = lax.rem(core + c, CORES)
                        to_chip = chip_at(off)
                        pltpu.make_async_remote_copy(
                            src_ref=src.at[rows, to_chip * CORES + to_core],
                            dst_ref=dst.at[rows, my_slots],
                            send_sem=send_sem.at[which],
                            recv_sem=recv_sem.at[which, i],
                            device_id=device(to_chip, to_core),
                            device_id_type=MESH,
                        ).start()
        return 0

    send_group(0, 0)

    for load in (*loads[:4], loads[6]):
        load.wait()
    gain[...] = 1.0 + norm_v[...].astype(F32).reshape(1, model_dim)
    n_blocks = n_steps // X_STEPS
    blk_rows = X_STEPS * num_rows

    def project(i, _):
        slot = lax.rem(i, 2)

        @pl.when(i + 1 < n_blocks)
        def _():
            x_load(i + 1, 1 - slot).start()

        x_load(i, slot).wait()
        x = x_blk[slot].reshape(blk_rows, model_dim).astype(F32)
        inv = lax.rsqrt(jnp.mean(x * x, axis=-1, keepdims=True) + NORM_EPS)
        normed = (x * inv * gain[...]).astype(BF16)
        out = pl.ds(pl.multiple_of(i * blk_rows, blk_rows), blk_rows)
        for j, w in enumerate((wq_v, wk_v, wv_v)):
            qkv[j, out, :] = jnp.dot(normed, w[...], preferred_element_type=F32).astype(BF16).astype(F32)
        return 0

    with jax.named_scope("project"):
        lax.fori_loop(0, n_blocks, project, 0)

    with jax.named_scope("w_hop1"):
        ring_turn(w_at, w_sems, 1, range(2))
    send_group(1, 0)

    def rope_row(b, _):
        step_id = lax.broadcasted_iota(jnp.int32, (n_steps, head_dim), 0)
        angle = (step_id + plen[b]).astype(F32) * freq[...]
        lane = lax.broadcasted_iota(jnp.int32, (n_steps, head_dim), 1)
        cos_part = jnp.cos(angle)
        sin_part = jnp.where(lane < head_dim // 2, -1.0, 1.0) * jnp.sin(angle)
        row = pl.ds(b, n_steps, stride=num_rows)

        def rotate(u):
            return u * cos_part + pltpu.roll(u, head_dim // 2, 1) * sin_part

        q_s[b] = (rotate(qkv[0, row, :]) * head_dim ** -0.5).astype(BF16)
        k_n[b] = rotate(qkv[1, row, :]).astype(BF16)
        v_n[b] = qkv[2, row, :].astype(BF16)
        for buf in (k_buf, v_buf):
            buf[b, seq_len:, :] = jnp.zeros((out_len - seq_len, head_dim), BF16)
        return 0

    with jax.named_scope("rope"):
        lax.fori_loop(0, num_rows, rope_row, 0)

    for hop in range(2, far):
        with jax.named_scope(f"w_hop{hop}"):
            ring_turn(w_at, w_sems, hop, range(2))
        send_group(hop, 0)
    with jax.named_scope(f"w_hop{far}"):
        ring_turn(w_at, w_sems, far, range(2))
    loads[4].wait()

    def to_sibling(off):
        view = w_all.at[:, my_lanes, my_share]
        return pltpu.make_async_remote_copy(
            src_ref=view, dst_ref=view, send_sem=dp_send, recv_sem=dp_recv,
            device_id=sibling(off), device_id_type=MESH)

    others_share = w_all.at[:, pl.ds(0, head_dim), pl.ds(0, (n_dp - 1) * share)]
    for off in range(1, n_dp):
        to_sibling(off).start()
    lax.fori_loop(far, n_groups, send_group, 0)

    w_swap = pltpu.make_async_remote_copy(
        src_ref=w_all.at[:, my_lanes], dst_ref=w_all.at[:, my_lanes], send_sem=p_send.at[BANDS], recv_sem=p_recv.at[BANDS],
        device_id=partner, device_id_type=MESH)

    def attend_row(b):
        start = plen[b]
        slot_id = lax.broadcasted_iota(jnp.int32, (out_len, n_steps), 0)
        step_id = lax.broadcasted_iota(jnp.int32, (out_len, n_steps), 1)
        pick = jnp.where(slot_id - step_id == start, 1.0, 0.0).astype(BF16)
        at = lax.broadcasted_iota(jnp.int32, (out_len, head_dim), 0) - start
        is_new = jnp.logical_and(at >= 0, at < n_steps)
        for buf, new in ((k_buf, k_n), (v_buf, v_n)):
            placed = jnp.dot(pick, new[b], preferred_element_type=F32)
            buf[b] = jnp.where(is_new, placed, buf[b].astype(F32)).astype(BF16)
        s = lax.dot_general(q_s[b], k_buf[b], (((1,), (1,)), ((), ())), preferred_element_type=F32)
        s_slot = lax.broadcasted_iota(jnp.int32, (n_steps, out_len), 1)
        s_step = lax.broadcasted_iota(jnp.int32, (n_steps, out_len), 0)
        s = jnp.where(s_slot - s_step <= start, s, -jnp.inf)
        e = jnp.exp(s - jnp.max(s, axis=-1, keepdims=True))
        a = (e / jnp.sum(e, axis=-1, keepdims=True)).astype(BF16)
        o = jnp.dot(a, v_buf[b], preferred_element_type=F32)
        o_sr[b // band, pl.ds(lax.rem(b, band), n_steps, stride=band), :] = o.astype(BF16).astype(F32)

    mine = pl.ds(pl.multiple_of(core * band_rows, band_rows), band_rows)
    theirs = pl.ds(pl.multiple_of(other * band_rows, band_rows), band_rows)
    o_sems = (o_send, o_recv)

    def swap(h):
        return pltpu.make_async_remote_copy(
            src_ref=o_snd.at[h], dst_ref=o_all.at[chip, pl.ds(h * band_rows, band_rows), my_lanes],
            send_sem=p_send.at[h], recv_sem=p_recv.at[h], device_id=partner, device_id_type=MESH)

    def swap_start(h):
        o_snd[h] = o_sr[h, theirs, :].astype(BF16)
        swap(h).start()
        o_all[chip, h * band_rows:(h + 1) * band_rows, my_lanes] = o_sr[h, mine, :].astype(BF16)

    def o_at(c, j):
        return o_all.at[c, pl.ds(j * piece, piece)]

    def band_pieces(h):
        return range(h * CUTS, (h + 1) * CUTS)

    def attend_group(i, _):
        rows = pl.ds(i * GROUP_ROWS, GROUP_ROWS)
        with jax.named_scope("wait_group"):
            for which, buf in enumerate((k_buf, v_buf)):
                wait_bytes(buf.at[rows, pl.ds(0, seq_len)], recv_sem.at[which, i])
        with jax.named_scope("attend_group"):
            for r in range(GROUP_ROWS):
                attend_row(i * GROUP_ROWS + r)

        @pl.when(i == n_groups // 2 - 1)
        def _():
            swap_start(0)

        @pl.when(i == n_groups // 2)
        def _():
            swap(0).wait_recv()
            ring_start(o_at, o_sems, 1, band_pieces(0))

        @pl.when(i == n_groups - 3)
        def _():
            if n_dp > 1:
                wait_bytes(others_share, dp_recv)
            w_swap.start()

        return 0

    lax.fori_loop(0, n_groups, attend_group, 0)

    def y_view(of_core, h, cols):
        return y_buf.at[pl.ds(pl.multiple_of(of_core * half_steps, half_steps), half_steps), pl.ds(h * band, band), cols]

    def hand_on(of_core, h, q):
        view = y_view(of_core, h, pl.ds(q * quarter, quarter))
        return pltpu.make_async_remote_copy(
            src_ref=view, dst_ref=view, send_sem=d_send.at[h], recv_sem=d_recv.at[h],
            device_id=partner, device_id_type=MESH)

    def y_add(h, froms, first=False, last=False):
        rows = slice(h * band_rows, (h + 1) * band_rows)
        for n in range(model_dim // wide):
            cols = slice(n * wide, (n + 1) * wide)
            total = None
            for off in froms:
                c = chip_at(off)
                part = jnp.dot(o_all[c, rows, :], w_all[c, :, cols], preferred_element_type=F32)
                total = part if total is None else total + part
            if first:
                total += x_res[:, h * band:(h + 1) * band, cols].astype(F32).reshape(band_rows, wide)
            else:
                total += y_acc[:, cols]
            if last:
                y_view(core, h, pl.ds(n * wide, wide))[...] = total.reshape(half_steps, band, wide).astype(BF16)
                if (n + 1) * wide % quarter == 0:
                    hand_on(core, h, n * wide // quarter).start()
            else:
                y_acc[:, cols] = total

    def turn(h, hop):
        with jax.named_scope(f"o_b{h}_hop{hop}"):
            ring_turn(o_at, o_sems, hop, band_pieces(h))

    def add(h, froms, **kwargs):
        with jax.named_scope(f"y_b{h}"):
            y_add(h, froms, **kwargs)

    near = [s * d for d in range(1, far - 1) for s in (1, -1)]
    edge = [far - 1, 1 - far]
    swap_start(1)
    turn(0, 1)
    with jax.named_scope("o_b1_start"):
        swap(1).wait_recv()
        ring_start(o_at, o_sems, 1, band_pieces(1))
    loads[5].wait()
    w_swap.wait_recv()
    for hop in range(2, far + 1):
        turn(0, hop)
        if hop == far - 2:
            add(0, [0] + near, first=True)
        if hop == far - 1:
            add(0, edge)
        if hop == far:
            add(0, [far], last=True)
        turn(1, hop - 1)
        if hop - 1 == far - 1:
            add(1, [0] + near + edge, first=True)
    turn(1, far)
    add(1, [far], last=True)

    with jax.named_scope("drain"):
        for which, buf in enumerate((k_buf, v_buf)):
            wait_bytes(buf.at[:, pl.ds(0, seq_len - slots)], send_sem.at[which])
        wait_bytes(w_all.at[pl.ds(0, chips - 1), pl.ds(0, head_dim), pl.ds(0, share)], w_send)
        wait_bytes(o_all.at[pl.ds(0, chips - 1)], o_send)
        if n_dp > 1:
            wait_bytes(others_share, dp_send)
        w_swap.wait_send()
        for h in range(BANDS):
            swap(h).wait_send()
            wait_bytes(y_view(core, h, pl.ds(0, model_dim)), d_send.at[h])
            wait_bytes(y_view(other, h, pl.ds(0, model_dim)), d_recv.at[h])


def write_kernel(k_buf, v_buf, y_buf, k_out, v_out, y_out, sem):
    parts = sem.shape[1]
    copies = []
    for a, (src, dst) in enumerate(((k_buf, k_out), (v_buf, v_out), (y_buf, y_out))):
        size = src.shape[0] // parts
        for i in range(parts):
            copies.append(pltpu.make_async_copy(src.at[pl.ds(i * size, size)], dst.at[pl.ds(i * size, size)], sem.at[a, i]))
    for copy in copies:
        copy.start()
    for copy in copies:
        copy.wait()


def solution(mesh):
    n_tp = mesh.shape["tp"]
    n_dp = mesh.shape["dp"]

    def local_block(k_cache, v_cache, prompt_len, x_steps, w_norm, w_q, w_k, w_v, w_o):
        num_rows, _, slots, head_dim = k_cache.shape
        n_steps, _, model_dim = x_steps.shape
        out_len = slots * n_tp + n_steps
        chips = n_tp // CORES
        far = chips // 2
        half_steps = n_steps // CORES
        half_rows = half_steps * num_rows
        wide = CORES * head_dim
        n_groups = num_rows // GROUP_ROWS
        pieces = BANDS * CUTS
        lanes = jnp.arange(head_dim, dtype=jnp.int32) % (head_dim // 2)
        freq = (ROPE_BASE ** (-2.0 * lanes.astype(F32) / head_dim)).reshape(1, head_dim)
        dma = pltpu.SemaphoreType.DMA
        in_hbm = functools.partial(pltpu.with_memory_space_constraint, memory_space=pltpu.HBM)

        def in_vmem(shape):
            return pltpu.VMEM(shape.shape, shape.dtype)

        hbm = pl.BlockSpec(memory_space=pltpu.HBM)
        vmem = pl.BlockSpec(memory_space=pltpu.VMEM)
        cache = jax.ShapeDtypeStruct((num_rows, out_len, head_dim), BF16)
        y_shape = jax.ShapeDtypeStruct(x_steps.shape, BF16)
        k_buf, v_buf, y_buf = pl.pallas_call(
            functools.partial(main_kernel, n_tp, n_dp),
            out_shape=(in_vmem(cache), in_vmem(cache), in_vmem(y_shape)),
            in_specs=[hbm, vmem] + [hbm] * 8,
            out_specs=(vmem, vmem, vmem),
            scratch_shapes=[
                pltpu.SMEM(prompt_len.shape, jnp.int32),
                pltpu.VMEM(w_norm.shape, BF16),
                pltpu.VMEM((1, model_dim), F32),
                pltpu.VMEM((model_dim, head_dim), BF16),
                pltpu.VMEM((model_dim, head_dim), BF16),
                pltpu.VMEM((model_dim, head_dim), BF16),
                pltpu.VMEM((2, X_STEPS, num_rows, model_dim), BF16),
                pltpu.VMEM((3, n_steps * num_rows, head_dim), F32),
                pltpu.VMEM((num_rows, n_steps, head_dim), BF16),
                pltpu.VMEM((num_rows, n_steps, head_dim), BF16),
                pltpu.VMEM((num_rows, n_steps, head_dim), BF16),
                pltpu.VMEM((BANDS, n_steps * num_rows // BANDS, head_dim), F32),
                pltpu.VMEM((BANDS, half_rows // BANDS, head_dim), BF16),
                pltpu.VMEM((chips, half_rows, wide), BF16),
                pltpu.VMEM((chips, wide, model_dim), BF16),
                pltpu.VMEM((half_steps, num_rows, model_dim), BF16),
                pltpu.VMEM((half_rows // BANDS, model_dim), F32),
                dma((7,)), dma((2,)),
                dma((2,)), dma((2, n_groups)),
                dma, dma((2, far, 2)),
                dma, dma,
                dma((BANDS + 1,)), dma((BANDS + 1,)),
                dma, dma((2, far, pieces)),
                dma((BANDS,)), dma((BANDS,)),
            ],
            compiler_params=pltpu.CompilerParams(collective_id=0, has_side_effects=True, vmem_limit_bytes=28 * 2**20),
            name="decode_block",
        )(in_hbm(prompt_len), freq, *map(in_hbm, (w_norm, k_cache, v_cache, x_steps, w_q, w_k, w_v, w_o)))
        k_out, v_out, y_out = pl.pallas_call(
            write_kernel,
            out_shape=(cache, cache, y_shape),
            in_specs=[vmem, vmem, vmem],
            out_specs=(hbm, hbm, hbm),
            scratch_shapes=[dma((3, 8))],
            compiler_params=pltpu.CompilerParams(vmem_limit_bytes=4 * 2**20),
            name="write_out",
        )(k_buf, v_buf, y_buf)
        return y_out, k_out[:, None], v_out[:, None]

    cache_spec = P("dp", None, "tp", None)
    col_spec = P(None, "tp")
    out_cache_spec = P("dp", "tp", None, None)
    return jax.shard_map(local_block, mesh=mesh, in_specs=(cache_spec, cache_spec, P("dp"), P(None, "dp", None), P(None), col_spec, col_spec, col_spec, P("tp", None)), out_specs=(P(None, "dp", None), out_cache_spec, out_cache_spec), check_vma=False)
```

```python
import functools

import jax
import jax.numpy as jnp
from jax import lax
from jax.experimental import pallas as pl
from jax.experimental.pallas import tpu as pltpu
from jax.sharding import PartitionSpec as P

ROPE_BASE = 10000.0
NORM_EPS = 1e-6
CORES = 2
GROUP_ROWS = 2
BANDS = 2
CUTS = 2
X_STEPS = 8
MESH = pl.DeviceIdType.MESH
BF16 = jnp.bfloat16
F32 = jnp.float32


def main_kernel(n_tp, n_dp, plen_in, freq, w_norm, k_in, v_in, x_in, w_q, w_k, w_v, w_o, k_buf, v_buf, y_buf,
                plen, norm_v, gain, wq_v, wk_v, wv_v, x_blk, qkv, q_s, k_n, v_n, o_sr, o_snd, o_all, w_all, x_res, y_acc,
                in_sem, x_sem, send_sem, recv_sem, w_send, w_recv, dp_send, dp_recv, p_send, p_recv,
                o_send, o_recv, d_send, d_recv):
    num_rows, out_len, head_dim = k_buf.shape
    n_steps, _, model_dim = x_in.shape
    slots = k_in.shape[2]
    seq_len = slots * n_tp
    chips = n_tp // CORES
    far = chips // 2
    half_steps = n_steps // CORES
    band = num_rows // BANDS
    band_rows = half_steps * band
    piece_steps = half_steps // CUTS
    piece = piece_steps * band
    wide = CORES * head_dim
    n_groups = num_rows // GROUP_ROWS
    share = model_dim // n_dp
    quarter = model_dim // 4

    dp = lax.axis_index("dp")
    me = lax.axis_index("tp")
    chip = me // CORES
    core = lax.rem(me, CORES)
    other = 1 - core

    def chip_at(offset):
        return lax.rem(chip + offset + chips, chips)

    def device(chip_index, core_index):
        return (dp, chip_index * CORES + core_index)

    def sibling(offset):
        return (lax.rem(dp + offset, n_dp), me)

    partner = device(chip, other)
    offsets = [0] + [s * d for d in range(1, far) for s in (1, -1)] + [far]
    my_lanes = pl.ds(pl.multiple_of(core * head_dim, head_dim), head_dim)

    barrier = pltpu.get_barrier_semaphore()
    for off in offsets:
        for c in range(CORES):
            if (off, c) != (0, 0):
                pl.semaphore_signal(barrier, inc=1, device_id=device(chip_at(off), lax.rem(core + c, CORES)), device_id_type=MESH)
    for off in range(1, n_dp):
        pl.semaphore_signal(barrier, inc=1, device_id=sibling(off), device_id_type=MESH)

    my_share = pl.ds(pl.multiple_of(dp * share, share), share)
    loads = [
        pltpu.make_async_copy(plen_in, plen, in_sem.at[0]),
        pltpu.make_async_copy(w_q, wq_v, in_sem.at[1]),
        pltpu.make_async_copy(w_k, wk_v, in_sem.at[2]),
        pltpu.make_async_copy(w_v, wv_v, in_sem.at[3]),
        pltpu.make_async_copy(w_o.at[:, my_share], w_all.at[chip, my_lanes, my_share], in_sem.at[4]),
        pltpu.make_async_copy(x_in.at[pl.ds(core * half_steps, half_steps)], x_res, in_sem.at[5]),
        pltpu.make_async_copy(w_norm, norm_v, in_sem.at[6]),
    ]
    for load in loads:
        load.start()

    def x_load(i, slot):
        return pltpu.make_async_copy(x_in.at[pl.ds(i * X_STEPS, X_STEPS)], x_blk.at[slot], x_sem.at[slot])

    x_load(0, 0).start()

    with jax.named_scope("barrier"):
        pl.semaphore_wait(barrier, n_tp - 1 + n_dp - 1)

    def hops(way, j):
        return far if (way + j) % 2 == 0 else far - 1

    def ring_copy(at, sems, way, hop, j, first=None):
        step = 1 if way == 0 else -1
        view = at(chip_at(-step * (hop - 1)), j)
        return pltpu.make_async_remote_copy(
            src_ref=view if first is None else first, dst_ref=view,
            send_sem=sems[0], recv_sem=sems[1].at[way, hop - 1, j],
            device_id=device(chip_at(step), core), device_id_type=MESH)

    def legs(hop, pieces):
        by_way = [sorted(pieces, key=lambda j, way=way: -hops(way, j)) for way in range(2)]
        return [(way, js[way]) for js in zip(*by_way) for way in range(2) if hop <= hops(way, js[way])]

    def ring_start(at, sems, hop, pieces):
        for way, j in legs(hop, pieces):
            ring_copy(at, sems, way, hop, j).start()

    def ring_turn(at, sems, hop, pieces):
        for way, j in legs(hop, pieces):
            ring_copy(at, sems, way, hop, j).wait_recv()
            if hop < hops(way, j):
                ring_copy(at, sems, way, hop + 1, j).start()

    def wait_bytes(view, sem):
        pltpu.make_async_copy(view, view, sem).wait()

    w_half = head_dim // 2
    w_sems = (w_send, w_recv)

    def w_at(c, j):
        return w_all.at[c, pl.ds(pl.multiple_of(core * head_dim, head_dim) + j * w_half, w_half), my_share]

    for way, j in legs(1, range(2)):
        ring_copy(w_at, w_sems, way, 1, j, w_o.at[pl.ds(j * w_half, w_half), my_share]).start()

    my_slots = pl.ds(pl.multiple_of(me * slots, slots), slots)

    def send_group(i, _):
        rows = pl.ds(i * GROUP_ROWS, GROUP_ROWS)
        for which, (src, dst) in enumerate(((k_in, k_buf), (v_in, v_buf))):
            pltpu.make_async_copy(src.at[rows, me], dst.at[rows, my_slots], recv_sem.at[which, i]).start()
            for c in range(CORES):
                for off in reversed(offsets):
                    if (off, c) != (0, 0):
                        to_core = lax.rem(core + c, CORES)
                        to_chip = chip_at(off)
                        pltpu.make_async_remote_copy(
                            src_ref=src.at[rows, to_chip * CORES + to_core],
                            dst_ref=dst.at[rows, my_slots],
                            send_sem=send_sem.at[which],
                            recv_sem=recv_sem.at[which, i],
                            device_id=device(to_chip, to_core),
                            device_id_type=MESH,
                        ).start()
        return 0

    send_group(0, 0)

    for load in (*loads[:4], loads[6]):
        load.wait()
    gain[...] = 1.0 + norm_v[...].astype(F32).reshape(1, model_dim)
    n_blocks = n_steps // X_STEPS
    blk_rows = X_STEPS * num_rows

    def project(i, _):
        slot = lax.rem(i, 2)

        @pl.when(i + 1 < n_blocks)
        def _():
            x_load(i + 1, 1 - slot).start()

        x_load(i, slot).wait()
        x = x_blk[slot].reshape(blk_rows, model_dim).astype(F32)
        inv = lax.rsqrt(jnp.mean(x * x, axis=-1, keepdims=True) + NORM_EPS)
        normed = (x * inv * gain[...]).astype(BF16)
        out = pl.ds(pl.multiple_of(i * blk_rows, blk_rows), blk_rows)
        for j, w in enumerate((wq_v, wk_v, wv_v)):
            qkv[j, out, :] = jnp.dot(normed, w[...], preferred_element_type=F32).astype(BF16).astype(F32)
        return 0

    with jax.named_scope("project"):
        lax.fori_loop(0, n_blocks, project, 0)

    with jax.named_scope("w_hop1"):
        ring_turn(w_at, w_sems, 1, range(2))
    send_group(1, 0)

    def rope_row(b, _):
        step_id = lax.broadcasted_iota(jnp.int32, (n_steps, head_dim), 0)
        angle = (step_id + plen[b]).astype(F32) * freq[...]
        lane = lax.broadcasted_iota(jnp.int32, (n_steps, head_dim), 1)
        cos_part = jnp.cos(angle)
        sin_part = jnp.where(lane < head_dim // 2, -1.0, 1.0) * jnp.sin(angle)
        row = pl.ds(b, n_steps, stride=num_rows)

        def rotate(u):
            return u * cos_part + pltpu.roll(u, head_dim // 2, 1) * sin_part

        q_s[b] = (rotate(qkv[0, row, :]) * head_dim ** -0.5).astype(BF16)
        k_n[b] = rotate(qkv[1, row, :]).astype(BF16)
        v_n[b] = qkv[2, row, :].astype(BF16)
        for buf in (k_buf, v_buf):
            buf[b, seq_len:, :] = jnp.zeros((out_len - seq_len, head_dim), BF16)
        return 0

    with jax.named_scope("rope"):
        lax.fori_loop(0, num_rows, rope_row, 0)

    for hop in range(2, far):
        with jax.named_scope(f"w_hop{hop}"):
            ring_turn(w_at, w_sems, hop, range(2))
        send_group(hop, 0)
    with jax.named_scope(f"w_hop{far}"):
        ring_turn(w_at, w_sems, far, range(2))
    loads[4].wait()

    def to_sibling(off):
        view = w_all.at[:, my_lanes, my_share]
        return pltpu.make_async_remote_copy(
            src_ref=view, dst_ref=view, send_sem=dp_send, recv_sem=dp_recv,
            device_id=sibling(off), device_id_type=MESH)

    others_share = w_all.at[:, pl.ds(0, head_dim), pl.ds(0, (n_dp - 1) * share)]
    for off in range(1, n_dp):
        to_sibling(off).start()
    lax.fori_loop(far, n_groups, send_group, 0)

    w_swap = pltpu.make_async_remote_copy(
        src_ref=w_all.at[:, my_lanes], dst_ref=w_all.at[:, my_lanes], send_sem=p_send.at[BANDS], recv_sem=p_recv.at[BANDS],
        device_id=partner, device_id_type=MESH)

    def attend_row(b):
        start = plen[b]
        slot_id = lax.broadcasted_iota(jnp.int32, (out_len, n_steps), 0)
        step_id = lax.broadcasted_iota(jnp.int32, (out_len, n_steps), 1)
        pick = jnp.where(slot_id - step_id == start, 1.0, 0.0).astype(BF16)
        at = lax.broadcasted_iota(jnp.int32, (out_len, head_dim), 0) - start
        is_new = jnp.logical_and(at >= 0, at < n_steps)
        for buf, new in ((k_buf, k_n), (v_buf, v_n)):
            placed = jnp.dot(pick, new[b], preferred_element_type=F32)
            buf[b] = jnp.where(is_new, placed, buf[b].astype(F32)).astype(BF16)
        s = lax.dot_general(q_s[b], k_buf[b], (((1,), (1,)), ((), ())), preferred_element_type=F32)
        s_slot = lax.broadcasted_iota(jnp.int32, (n_steps, out_len), 1)
        s_step = lax.broadcasted_iota(jnp.int32, (n_steps, out_len), 0)
        s = jnp.where(s_slot - s_step <= start, s, -jnp.inf)
        e = jnp.exp(s - jnp.max(s, axis=-1, keepdims=True))
        a = (e / jnp.sum(e, axis=-1, keepdims=True)).astype(BF16)
        o = jnp.dot(a, v_buf[b], preferred_element_type=F32)
        o_sr[b // band, pl.ds(lax.rem(b, band), n_steps, stride=band), :] = o.astype(BF16).astype(F32)

    mine = pl.ds(pl.multiple_of(core * band_rows, band_rows), band_rows)
    theirs = pl.ds(pl.multiple_of(other * band_rows, band_rows), band_rows)
    o_sems = (o_send, o_recv)

    def swap(h):
        return pltpu.make_async_remote_copy(
            src_ref=o_snd.at[h], dst_ref=o_all.at[chip, pl.ds(h * band_rows, band_rows), my_lanes],
            send_sem=p_send.at[h], recv_sem=p_recv.at[h], device_id=partner, device_id_type=MESH)

    def swap_start(h):
        o_snd[h] = o_sr[h, theirs, :].astype(BF16)
        swap(h).start()
        o_all[chip, h * band_rows:(h + 1) * band_rows, my_lanes] = o_sr[h, mine, :].astype(BF16)

    def o_at(c, j):
        return o_all.at[c, pl.ds(j * piece, piece)]

    def band_pieces(h):
        return range(h * CUTS, (h + 1) * CUTS)

    def attend_group(i, _):
        rows = pl.ds(i * GROUP_ROWS, GROUP_ROWS)
        with jax.named_scope("wait_group"):
            for which, buf in enumerate((k_buf, v_buf)):
                wait_bytes(buf.at[rows, pl.ds(0, seq_len)], recv_sem.at[which, i])
        with jax.named_scope("attend_group"):
            for r in range(GROUP_ROWS):
                attend_row(i * GROUP_ROWS + r)

        @pl.when(i == n_groups // 2 - 1)
        def _():
            swap_start(0)

        @pl.when(i == n_groups // 2)
        def _():
            swap(0).wait_recv()
            ring_start(o_at, o_sems, 1, band_pieces(0))

        @pl.when(i == n_groups - 3)
        def _():
            if n_dp > 1:
                wait_bytes(others_share, dp_recv)
            w_swap.start()

        return 0

    lax.fori_loop(0, n_groups, attend_group, 0)

    def y_view(of_core, h, cols):
        return y_buf.at[pl.ds(pl.multiple_of(of_core * half_steps, half_steps), half_steps), pl.ds(h * band, band), cols]

    def hand_on(of_core, h, q):
        view = y_view(of_core, h, pl.ds(q * quarter, quarter))
        return pltpu.make_async_remote_copy(
            src_ref=view, dst_ref=view, send_sem=d_send.at[h], recv_sem=d_recv.at[h],
            device_id=partner, device_id_type=MESH)

    def y_add(h, froms, first=False, last=False):
        rows = slice(h * band_rows, (h + 1) * band_rows)
        for n in range(model_dim // wide):
            cols = slice(n * wide, (n + 1) * wide)
            total = None
            for off in froms:
                c = chip_at(off)
                part = jnp.dot(o_all[c, rows, :], w_all[c, :, cols], preferred_element_type=F32)
                total = part if total is None else total + part
            if first:
                total += x_res[:, h * band:(h + 1) * band, cols].astype(F32).reshape(band_rows, wide)
            else:
                total += y_acc[:, cols]
            if last:
                y_view(core, h, pl.ds(n * wide, wide))[...] = total.reshape(half_steps, band, wide).astype(BF16)
                if (n + 1) * wide % quarter == 0:
                    hand_on(core, h, n * wide // quarter).start()
            else:
                y_acc[:, cols] = total

    def turn(h, hop):
        with jax.named_scope(f"o_b{h}_hop{hop}"):
            ring_turn(o_at, o_sems, hop, band_pieces(h))

    def add(h, froms, **kwargs):
        with jax.named_scope(f"y_b{h}"):
            y_add(h, froms, **kwargs)

    near = [s * d for d in range(1, far - 1) for s in (1, -1)]
    edge = [far - 1, 1 - far]
    swap_start(1)
    turn(0, 1)
    with jax.named_scope("o_b1_start"):
        swap(1).wait_recv()
        ring_start(o_at, o_sems, 1, band_pieces(1))
    loads[5].wait()
    w_swap.wait_recv()
    for hop in range(2, far + 1):
        turn(0, hop)
        if hop == far - 2:
            add(0, [0] + near, first=True)
        if hop == far - 1:
            add(0, edge)
        if hop == far:
            add(0, [far], last=True)
        turn(1, hop - 1)
        if hop - 1 == far - 1:
            add(1, [0] + near + edge, first=True)
    turn(1, far)
    add(1, [far], last=True)

    with jax.named_scope("drain"):
        for which, buf in enumerate((k_buf, v_buf)):
            wait_bytes(buf.at[:, pl.ds(0, seq_len - slots)], send_sem.at[which])
        wait_bytes(w_all.at[pl.ds(0, chips - 1), pl.ds(0, head_dim), pl.ds(0, share)], w_send)
        wait_bytes(o_all.at[pl.ds(0, chips - 1)], o_send)
        if n_dp > 1:
            wait_bytes(others_share, dp_send)
        w_swap.wait_send()
        for h in range(BANDS):
            swap(h).wait_send()
            wait_bytes(y_view(core, h, pl.ds(0, model_dim)), d_send.at[h])
            wait_bytes(y_view(other, h, pl.ds(0, model_dim)), d_recv.at[h])


def write_kernel(k_buf, v_buf, y_buf, k_out, v_out, y_out, sem):
    parts = sem.shape[1]
    copies = []
    for a, (src, dst) in enumerate(((k_buf, k_out), (v_buf, v_out), (y_buf, y_out))):
        size = src.shape[0] // parts
        for i in range(parts):
            copies.append(pltpu.make_async_copy(src.at[pl.ds(i * size, size)], dst.at[pl.ds(i * size, size)], sem.at[a, i]))
    for copy in copies:
        copy.start()
    for copy in copies:
        copy.wait()


def solution(mesh):
    n_tp = mesh.shape["tp"]
    n_dp = mesh.shape["dp"]

    def local_block(k_cache, v_cache, prompt_len, x_steps, w_norm, w_q, w_k, w_v, w_o):
        num_rows, _, slots, head_dim = k_cache.shape
        n_steps, _, model_dim = x_steps.shape
        out_len = slots * n_tp + n_steps
        chips = n_tp // CORES
        far = chips // 2
        half_steps = n_steps // CORES
        half_rows = half_steps * num_rows
        wide = CORES * head_dim
        n_groups = num_rows // GROUP_ROWS
        pieces = BANDS * CUTS
        lanes = jnp.arange(head_dim, dtype=jnp.int32) % (head_dim // 2)
        freq = (ROPE_BASE ** (-2.0 * lanes.astype(F32) / head_dim)).reshape(1, head_dim)
        dma = pltpu.SemaphoreType.DMA
        in_hbm = functools.partial(pltpu.with_memory_space_constraint, memory_space=pltpu.HBM)

        def in_vmem(shape):
            return pltpu.VMEM(shape.shape, shape.dtype)

        hbm = pl.BlockSpec(memory_space=pltpu.HBM)
        vmem = pl.BlockSpec(memory_space=pltpu.VMEM)
        cache = jax.ShapeDtypeStruct((num_rows, out_len, head_dim), BF16)
        y_shape = jax.ShapeDtypeStruct(x_steps.shape, BF16)
        k_buf, v_buf, y_buf = pl.pallas_call(
            functools.partial(main_kernel, n_tp, n_dp),
            out_shape=(in_vmem(cache), in_vmem(cache), in_vmem(y_shape)),
            in_specs=[hbm, vmem] + [hbm] * 8,
            out_specs=(vmem, vmem, vmem),
            scratch_shapes=[
                pltpu.SMEM(prompt_len.shape, jnp.int32),
                pltpu.VMEM(w_norm.shape, BF16),
                pltpu.VMEM((1, model_dim), F32),
                pltpu.VMEM((model_dim, head_dim), BF16),
                pltpu.VMEM((model_dim, head_dim), BF16),
                pltpu.VMEM((model_dim, head_dim), BF16),
                pltpu.VMEM((2, X_STEPS, num_rows, model_dim), BF16),
                pltpu.VMEM((3, n_steps * num_rows, head_dim), F32),
                pltpu.VMEM((num_rows, n_steps, head_dim), BF16),
                pltpu.VMEM((num_rows, n_steps, head_dim), BF16),
                pltpu.VMEM((num_rows, n_steps, head_dim), BF16),
                pltpu.VMEM((BANDS, n_steps * num_rows // BANDS, head_dim), F32),
                pltpu.VMEM((BANDS, half_rows // BANDS, head_dim), BF16),
                pltpu.VMEM((chips, half_rows, wide), BF16),
                pltpu.VMEM((chips, wide, model_dim), BF16),
                pltpu.VMEM((half_steps, num_rows, model_dim), BF16),
                pltpu.VMEM((half_rows // BANDS, model_dim), F32),
                dma((7,)), dma((2,)),
                dma((2,)), dma((2, n_groups)),
                dma, dma((2, far, 2)),
                dma, dma,
                dma((BANDS + 1,)), dma((BANDS + 1,)),
                dma, dma((2, far, pieces)),
                dma((BANDS,)), dma((BANDS,)),
            ],
            compiler_params=pltpu.CompilerParams(collective_id=0, has_side_effects=True, vmem_limit_bytes=28 * 2**20),
            name="decode_block",
        )(in_hbm(prompt_len), freq, *map(in_hbm, (w_norm, k_cache, v_cache, x_steps, w_q, w_k, w_v, w_o)))
        k_out, v_out, y_out = pl.pallas_call(
            write_kernel,
            out_shape=(cache, cache, y_shape),
            in_specs=[vmem, vmem, vmem],
            out_specs=(hbm, hbm, hbm),
            scratch_shapes=[dma((3, 8))],
            compiler_params=pltpu.CompilerParams(vmem_limit_bytes=4 * 2**20),
            name="write_out",
        )(k_buf, v_buf, y_buf)
        return y_out, k_out[:, None], v_out[:, None]

    cache_spec = P("dp", None, "tp", None)
    col_spec = P(None, "tp")
    out_cache_spec = P("dp", "tp", None, None)
    return jax.shard_map(local_block, mesh=mesh, in_specs=(cache_spec, cache_spec, P("dp"), P(None, "dp", None), P(None), col_spec, col_spec, col_spec, P("tp", None)), out_specs=(P(None, "dp", None), out_cache_spec, out_cache_spec), check_vma=False)
```

```python
import functools

import jax
import jax.numpy as jnp
from jax import lax
from jax.experimental import pallas as pl
from jax.experimental.pallas import tpu as pltpu
from jax.sharding import PartitionSpec as P

ROPE_BASE = 10000.0
NORM_EPS = 1e-6
CORES = 2
GROUP_ROWS = 2
BANDS = 2
CUTS = 2
X_STEPS = 8
MESH = pl.DeviceIdType.MESH
BF16 = jnp.bfloat16
F32 = jnp.float32


def main_kernel(n_tp, n_dp, plen_in, freq, w_norm, k_in, v_in, x_in, w_q, w_k, w_v, w_o, k_buf, v_buf, y_buf,
                plen, norm_v, gain, wq_v, wk_v, wv_v, x_blk, qkv, q_s, k_n, v_n, o_sr, o_snd, o_all, w_all, x_res, y_acc,
                in_sem, x_sem, send_sem, recv_sem, w_send, w_recv, dp_send, dp_recv, p_send, p_recv,
                o_send, o_recv, d_send, d_recv):
    num_rows, out_len, head_dim = k_buf.shape
    n_steps, _, model_dim = x_in.shape
    slots = k_in.shape[2]
    seq_len = slots * n_tp
    chips = n_tp // CORES
    far = chips // 2
    half_steps = n_steps // CORES
    band = num_rows // BANDS
    band_rows = half_steps * band
    piece_steps = half_steps // CUTS
    piece = piece_steps * band
    wide = CORES * head_dim
    n_groups = num_rows // GROUP_ROWS
    share = model_dim // n_dp
    quarter = model_dim // 4

    dp = lax.axis_index("dp")
    me = lax.axis_index("tp")
    chip = me // CORES
    core = lax.rem(me, CORES)
    other = 1 - core

    def chip_at(offset):
        return lax.rem(chip + offset + chips, chips)

    def device(chip_index, core_index):
        return (dp, chip_index * CORES + core_index)

    def sibling(offset):
        return (lax.rem(dp + offset, n_dp), me)

    partner = device(chip, other)
    offsets = [0] + [s * d for d in range(1, far) for s in (1, -1)] + [far]
    my_lanes = pl.ds(pl.multiple_of(core * head_dim, head_dim), head_dim)

    barrier = pltpu.get_barrier_semaphore()
    for off in offsets:
        for c in range(CORES):
            if (off, c) != (0, 0):
                pl.semaphore_signal(barrier, inc=1, device_id=device(chip_at(off), lax.rem(core + c, CORES)), device_id_type=MESH)
    for off in range(1, n_dp):
        pl.semaphore_signal(barrier, inc=1, device_id=sibling(off), device_id_type=MESH)

    my_share = pl.ds(pl.multiple_of(dp * share, share), share)
    loads = [
        pltpu.make_async_copy(plen_in, plen, in_sem.at[0]),
        pltpu.make_async_copy(w_q, wq_v, in_sem.at[1]),
        pltpu.make_async_copy(w_k, wk_v, in_sem.at[2]),
        pltpu.make_async_copy(w_v, wv_v, in_sem.at[3]),
        pltpu.make_async_copy(w_o.at[:, my_share], w_all.at[chip, my_lanes, my_share], in_sem.at[4]),
        pltpu.make_async_copy(x_in.at[pl.ds(core * half_steps, half_steps)], x_res, in_sem.at[5]),
        pltpu.make_async_copy(w_norm, norm_v, in_sem.at[6]),
    ]
    for load in loads:
        load.start()

    def x_load(i, slot):
        return pltpu.make_async_copy(x_in.at[pl.ds(i * X_STEPS, X_STEPS)], x_blk.at[slot], x_sem.at[slot])

    x_load(0, 0).start()

    with jax.named_scope("barrier"):
        pl.semaphore_wait(barrier, n_tp - 1 + n_dp - 1)

    def hops(way, j):
        return far if (way + j) % 2 == 0 else far - 1

    def ring_copy(at, sems, way, hop, j, first=None):
        step = 1 if way == 0 else -1
        view = at(chip_at(-step * (hop - 1)), j)
        return pltpu.make_async_remote_copy(
            src_ref=view if first is None else first, dst_ref=view,
            send_sem=sems[0], recv_sem=sems[1].at[way, hop - 1, j],
            device_id=device(chip_at(step), core), device_id_type=MESH)

    def legs(hop, pieces):
        by_way = [sorted(pieces, key=lambda j, way=way: -hops(way, j)) for way in range(2)]
        return [(way, js[way]) for js in zip(*by_way) for way in range(2) if hop <= hops(way, js[way])]

    def ring_turn(at, sems, hop, pieces):
        for way, j in legs(hop, pieces):
            ring_copy(at, sems, way, hop, j).wait_recv()
            if hop < hops(way, j):
                ring_copy(at, sems, way, hop + 1, j).start()

    def wait_bytes(view, sem):
        pltpu.make_async_copy(view, view, sem).wait()

    w_half = head_dim // 2
    w_sems = (w_send, w_recv)

    def w_at(c, j):
        return w_all.at[c, pl.ds(pl.multiple_of(core * head_dim, head_dim) + j * w_half, w_half), my_share]

    for way, j in legs(1, range(2)):
        ring_copy(w_at, w_sems, way, 1, j, w_o.at[pl.ds(j * w_half, w_half), my_share]).start()

    my_slots = pl.ds(pl.multiple_of(me * slots, slots), slots)

    def send_group(i, _):
        rows = pl.ds(i * GROUP_ROWS, GROUP_ROWS)
        for which, (src, dst) in enumerate(((k_in, k_buf), (v_in, v_buf))):
            pltpu.make_async_copy(src.at[rows, me], dst.at[rows, my_slots], recv_sem.at[which, i]).start()
            for c in range(CORES):
                for off in reversed(offsets):
                    if (off, c) != (0, 0):
                        to_core = lax.rem(core + c, CORES)
                        to_chip = chip_at(off)
                        pltpu.make_async_remote_copy(
                            src_ref=src.at[rows, to_chip * CORES + to_core],
                            dst_ref=dst.at[rows, my_slots],
                            send_sem=send_sem.at[which],
                            recv_sem=recv_sem.at[which, i],
                            device_id=device(to_chip, to_core),
                            device_id_type=MESH,
                        ).start()
        return 0

    send_group(0, 0)

    for load in (*loads[:4], loads[6]):
        load.wait()
    gain[...] = 1.0 + norm_v[...].astype(F32).reshape(1, model_dim)
    n_blocks = n_steps // X_STEPS
    blk_rows = X_STEPS * num_rows

    def project(i, _):
        slot = lax.rem(i, 2)

        @pl.when(i + 1 < n_blocks)
        def _():
            x_load(i + 1, 1 - slot).start()

        x_load(i, slot).wait()
        x = x_blk[slot].reshape(blk_rows, model_dim).astype(F32)
        inv = lax.rsqrt(jnp.mean(x * x, axis=-1, keepdims=True) + NORM_EPS)
        normed = (x * inv * gain[...]).astype(BF16)
        out = pl.ds(pl.multiple_of(i * blk_rows, blk_rows), blk_rows)
        for j, w in enumerate((wq_v, wk_v, wv_v)):
            qkv[j, out, :] = jnp.dot(normed, w[...], preferred_element_type=F32).astype(BF16).astype(F32)
        return 0

    with jax.named_scope("project"):
        lax.fori_loop(0, n_blocks, project, 0)

    with jax.named_scope("w_hop1"):
        ring_turn(w_at, w_sems, 1, range(2))
    send_group(1, 0)

    def rope_row(b, _):
        step_id = lax.broadcasted_iota(jnp.int32, (n_steps, head_dim), 0)
        angle = (step_id + plen[b]).astype(F32) * freq[...]
        lane = lax.broadcasted_iota(jnp.int32, (n_steps, head_dim), 1)
        cos_part = jnp.cos(angle)
        sin_part = jnp.where(lane < head_dim // 2, -1.0, 1.0) * jnp.sin(angle)
        row = pl.ds(b, n_steps, stride=num_rows)

        def rotate(u):
            return u * cos_part + pltpu.roll(u, head_dim // 2, 1) * sin_part

        q_s[b] = (rotate(qkv[0, row, :]) * head_dim ** -0.5).astype(BF16)
        k_n[b] = rotate(qkv[1, row, :]).astype(BF16)
        v_n[b] = qkv[2, row, :].astype(BF16)
        for buf in (k_buf, v_buf):
            buf[b, seq_len:, :] = jnp.zeros((out_len - seq_len, head_dim), BF16)
        return 0

    with jax.named_scope("rope"):
        lax.fori_loop(0, num_rows, rope_row, 0)

    for hop in range(2, far):
        with jax.named_scope(f"w_hop{hop}"):
            ring_turn(w_at, w_sems, hop, range(2))
        send_group(hop, 0)
    with jax.named_scope(f"w_hop{far}"):
        ring_turn(w_at, w_sems, far, range(2))
    loads[4].wait()

    def to_sibling(off):
        view = w_all.at[:, my_lanes, my_share]
        return pltpu.make_async_remote_copy(
            src_ref=view, dst_ref=view, send_sem=dp_send, recv_sem=dp_recv,
            device_id=sibling(off), device_id_type=MESH)

    others_share = w_all.at[:, pl.ds(0, head_dim), pl.ds(0, (n_dp - 1) * share)]
    for off in range(1, n_dp):
        to_sibling(off).start()
    lax.fori_loop(far, n_groups, send_group, 0)

    w_swap = pltpu.make_async_remote_copy(
        src_ref=w_all.at[:, my_lanes], dst_ref=w_all.at[:, my_lanes], send_sem=p_send.at[BANDS], recv_sem=p_recv.at[BANDS],
        device_id=partner, device_id_type=MESH)

    def attend_row(b):
        start = plen[b]
        slot_id = lax.broadcasted_iota(jnp.int32, (out_len, n_steps), 0)
        step_id = lax.broadcasted_iota(jnp.int32, (out_len, n_steps), 1)
        pick = jnp.where(slot_id - step_id == start, 1.0, 0.0).astype(BF16)
        at = lax.broadcasted_iota(jnp.int32, (out_len, head_dim), 0) - start
        is_new = jnp.logical_and(at >= 0, at < n_steps)
        for buf, new in ((k_buf, k_n), (v_buf, v_n)):
            placed = jnp.dot(pick, new[b], preferred_element_type=F32)
            buf[b] = jnp.where(is_new, placed, buf[b].astype(F32)).astype(BF16)
        s = lax.dot_general(q_s[b], k_buf[b], (((1,), (1,)), ((), ())), preferred_element_type=F32)
        s_slot = lax.broadcasted_iota(jnp.int32, (n_steps, out_len), 1)
        s_step = lax.broadcasted_iota(jnp.int32, (n_steps, out_len), 0)
        s = jnp.where(s_slot - s_step <= start, s, -jnp.inf)
        e = jnp.exp(s - jnp.max(s, axis=-1, keepdims=True))
        a = (e / jnp.sum(e, axis=-1, keepdims=True)).astype(BF16)
        o = jnp.dot(a, v_buf[b], preferred_element_type=F32)
        o_sr[b // band, pl.ds(lax.rem(b, band), n_steps, stride=band), :] = o.astype(BF16).astype(F32)

    mine = pl.ds(pl.multiple_of(core * band_rows, band_rows), band_rows)
    theirs = pl.ds(pl.multiple_of(other * band_rows, band_rows), band_rows)
    o_sems = (o_send, o_recv)

    def swap(h):
        return pltpu.make_async_remote_copy(
            src_ref=o_snd.at[h], dst_ref=o_all.at[chip, pl.ds(h * band_rows, band_rows), my_lanes],
            send_sem=p_send.at[h], recv_sem=p_recv.at[h], device_id=partner, device_id_type=MESH)

    def swap_start(h):
        o_snd[h] = o_sr[h, theirs, :].astype(BF16)
        swap(h).start()
        o_all[chip, h * band_rows:(h + 1) * band_rows, my_lanes] = o_sr[h, mine, :].astype(BF16)

    def o_at(c, j):
        return o_all.at[c, pl.ds(j * piece, piece)]

    def band_pieces(h):
        return range(h * CUTS, (h + 1) * CUTS)

    def o_start(h):
        swap_start(h)
        for way, j in legs(1, band_pieces(h)):
            view = o_all.at[chip, pl.ds(j * piece, piece), my_lanes]
            for to_core, src in ((core, view), (other, o_snd.at[h, pl.ds(j % CUTS * piece, piece)])):
                pltpu.make_async_remote_copy(
                    src_ref=src, dst_ref=view, send_sem=o_send, recv_sem=o_recv.at[way, 0, j],
                    device_id=device(chip_at(1 if way == 0 else -1), to_core), device_id_type=MESH).start()

    def attend_group(i, _):
        rows = pl.ds(i * GROUP_ROWS, GROUP_ROWS)
        with jax.named_scope("wait_group"):
            for which, buf in enumerate((k_buf, v_buf)):
                wait_bytes(buf.at[rows, pl.ds(0, seq_len)], recv_sem.at[which, i])
        with jax.named_scope("attend_group"):
            for r in range(GROUP_ROWS):
                attend_row(i * GROUP_ROWS + r)

        @pl.when(i == n_groups // 2 - 1)
        def _():
            o_start(0)

        @pl.when(i == n_groups - 3)
        def _():
            if n_dp > 1:
                wait_bytes(others_share, dp_recv)
            w_swap.start()

        return 0

    lax.fori_loop(0, n_groups, attend_group, 0)

    def y_view(of_core, h, cols):
        return y_buf.at[pl.ds(pl.multiple_of(of_core * half_steps, half_steps), half_steps), pl.ds(h * band, band), cols]

    def hand_on(of_core, h, q):
        view = y_view(of_core, h, pl.ds(q * quarter, quarter))
        return pltpu.make_async_remote_copy(
            src_ref=view, dst_ref=view, send_sem=d_send.at[h], recv_sem=d_recv.at[h],
            device_id=partner, device_id_type=MESH)

    def y_add(h, froms, first=False, last=False):
        rows = slice(h * band_rows, (h + 1) * band_rows)
        for n in range(model_dim // wide):
            cols = slice(n * wide, (n + 1) * wide)
            total = None
            for off in froms:
                c = chip_at(off)
                part = jnp.dot(o_all[c, rows, :], w_all[c, :, cols], preferred_element_type=F32)
                total = part if total is None else total + part
            if first:
                total += x_res[:, h * band:(h + 1) * band, cols].astype(F32).reshape(band_rows, wide)
            else:
                total += y_acc[h, :, cols]
            if last:
                y_view(core, h, pl.ds(n * wide, wide))[...] = total.reshape(half_steps, band, wide).astype(BF16)
                if (n + 1) * wide % quarter == 0:
                    hand_on(core, h, n * wide // quarter).start()
            else:
                y_acc[h, :, cols] = total

    def turn(h, hop):
        with jax.named_scope(f"o_b{h}_hop{hop}"):
            ring_turn(o_at, o_sems, hop, band_pieces(h))

    def add(h, froms, **kwargs):
        with jax.named_scope(f"y_b{h}"):
            y_add(h, froms, **kwargs)

    near = [s * d for d in range(1, far - 1) for s in (1, -1)]
    edge = [far - 1, 1 - far]
    o_start(1)
    turn(0, 1)
    turn(1, 1)
    for hop in range(2, far + 1):
        turn(0, hop)
        if hop == far - 2:
            loads[5].wait()
            w_swap.wait_recv()
            for h in range(BANDS):
                swap(h).wait_recv()
            add(0, [0] + near, first=True)
        if hop == far - 1:
            add(0, edge)
            add(1, [0] + near, first=True)
        if hop == far:
            add(0, [far], last=True)
        turn(1, hop)
        if hop == far - 1:
            add(1, edge)
    add(1, [far], last=True)

    with jax.named_scope("drain"):
        for which, buf in enumerate((k_buf, v_buf)):
            wait_bytes(buf.at[:, pl.ds(0, seq_len - slots)], send_sem.at[which])
        wait_bytes(w_all.at[pl.ds(0, chips - 1), pl.ds(0, head_dim), pl.ds(0, share)], w_send)
        wait_bytes(o_all.at[pl.ds(0, chips - 1)], o_send)
        if n_dp > 1:
            wait_bytes(others_share, dp_send)
        w_swap.wait_send()
        for h in range(BANDS):
            swap(h).wait_send()
            wait_bytes(y_view(core, h, pl.ds(0, model_dim)), d_send.at[h])
            wait_bytes(y_view(other, h, pl.ds(0, model_dim)), d_recv.at[h])


def write_kernel(k_buf, v_buf, y_buf, k_out, v_out, y_out, sem):
    parts = sem.shape[1]
    copies = []
    for a, (src, dst) in enumerate(((k_buf, k_out), (v_buf, v_out), (y_buf, y_out))):
        size = src.shape[0] // parts
        for i in range(parts):
            copies.append(pltpu.make_async_copy(src.at[pl.ds(i * size, size)], dst.at[pl.ds(i * size, size)], sem.at[a, i]))
    for copy in copies:
        copy.start()
    for copy in copies:
        copy.wait()


def solution(mesh):
    n_tp = mesh.shape["tp"]
    n_dp = mesh.shape["dp"]

    def local_block(k_cache, v_cache, prompt_len, x_steps, w_norm, w_q, w_k, w_v, w_o):
        num_rows, _, slots, head_dim = k_cache.shape
        n_steps, _, model_dim = x_steps.shape
        out_len = slots * n_tp + n_steps
        chips = n_tp // CORES
        far = chips // 2
        half_steps = n_steps // CORES
        half_rows = half_steps * num_rows
        wide = CORES * head_dim
        n_groups = num_rows // GROUP_ROWS
        pieces = BANDS * CUTS
        lanes = jnp.arange(head_dim, dtype=jnp.int32) % (head_dim // 2)
        freq = (ROPE_BASE ** (-2.0 * lanes.astype(F32) / head_dim)).reshape(1, head_dim)
        dma = pltpu.SemaphoreType.DMA
        in_hbm = functools.partial(pltpu.with_memory_space_constraint, memory_space=pltpu.HBM)

        def in_vmem(shape):
            return pltpu.VMEM(shape.shape, shape.dtype)

        hbm = pl.BlockSpec(memory_space=pltpu.HBM)
        vmem = pl.BlockSpec(memory_space=pltpu.VMEM)
        cache = jax.ShapeDtypeStruct((num_rows, out_len, head_dim), BF16)
        y_shape = jax.ShapeDtypeStruct(x_steps.shape, BF16)
        k_buf, v_buf, y_buf = pl.pallas_call(
            functools.partial(main_kernel, n_tp, n_dp),
            out_shape=(in_vmem(cache), in_vmem(cache), in_vmem(y_shape)),
            in_specs=[hbm, vmem] + [hbm] * 8,
            out_specs=(vmem, vmem, vmem),
            scratch_shapes=[
                pltpu.SMEM(prompt_len.shape, jnp.int32),
                pltpu.VMEM(w_norm.shape, BF16),
                pltpu.VMEM((1, model_dim), F32),
                pltpu.VMEM((model_dim, head_dim), BF16),
                pltpu.VMEM((model_dim, head_dim), BF16),
                pltpu.VMEM((model_dim, head_dim), BF16),
                pltpu.VMEM((2, X_STEPS, num_rows, model_dim), BF16),
                pltpu.VMEM((3, n_steps * num_rows, head_dim), F32),
                pltpu.VMEM((num_rows, n_steps, head_dim), BF16),
                pltpu.VMEM((num_rows, n_steps, head_dim), BF16),
                pltpu.VMEM((num_rows, n_steps, head_dim), BF16),
                pltpu.VMEM((BANDS, n_steps * num_rows // BANDS, head_dim), F32),
                pltpu.VMEM((BANDS, half_rows // BANDS, head_dim), BF16),
                pltpu.VMEM((chips, half_rows, wide), BF16),
                pltpu.VMEM((chips, wide, model_dim), BF16),
                pltpu.VMEM((half_steps, num_rows, model_dim), BF16),
                pltpu.VMEM((BANDS, half_rows // BANDS, model_dim), F32),
                dma((7,)), dma((2,)),
                dma((2,)), dma((2, n_groups)),
                dma, dma((2, far, 2)),
                dma, dma,
                dma((BANDS + 1,)), dma((BANDS + 1,)),
                dma, dma((2, far, pieces)),
                dma((BANDS,)), dma((BANDS,)),
            ],
            compiler_params=pltpu.CompilerParams(collective_id=0, has_side_effects=True, vmem_limit_bytes=28 * 2**20),
            name="decode_block",
        )(in_hbm(prompt_len), freq, *map(in_hbm, (w_norm, k_cache, v_cache, x_steps, w_q, w_k, w_v, w_o)))
        k_out, v_out, y_out = pl.pallas_call(
            write_kernel,
            out_shape=(cache, cache, y_shape),
            in_specs=[vmem, vmem, vmem],
            out_specs=(hbm, hbm, hbm),
            scratch_shapes=[dma((3, 8))],
            compiler_params=pltpu.CompilerParams(vmem_limit_bytes=4 * 2**20),
            name="write_out",
        )(k_buf, v_buf, y_buf)
        return y_out, k_out[:, None], v_out[:, None]

    cache_spec = P("dp", None, "tp", None)
    col_spec = P(None, "tp")
    out_cache_spec = P("dp", "tp", None, None)
    return jax.shard_map(local_block, mesh=mesh, in_specs=(cache_spec, cache_spec, P("dp"), P(None, "dp", None), P(None), col_spec, col_spec, col_spec, P("tp", None)), out_specs=(P(None, "dp", None), out_cache_spec, out_cache_spec), check_vma=False)
```

```python
import functools

import jax
import jax.numpy as jnp
from jax import lax
from jax.experimental import pallas as pl
from jax.experimental.pallas import tpu as pltpu
from jax.sharding import PartitionSpec as P

ROPE_BASE = 10000.0
NORM_EPS = 1e-6
CORES = 2
GROUP_ROWS = 2
BANDS = 2
CUTS = 2
X_STEPS = 8
MESH = pl.DeviceIdType.MESH
BF16 = jnp.bfloat16
F32 = jnp.float32


def main_kernel(n_tp, n_dp, plen_in, freq, w_norm, k_in, v_in, x_in, w_q, w_k, w_v, w_o, k_buf, v_buf, y_buf, o_all, w_all, o_oth, y_acc,
                plen, norm_v, gain, wq_v, wk_v, wv_v, x_blk, qkv, q_s, k_n, v_n, o_sr, o_snd, x_res, x_oth,
                in_sem, x_sem, send_sem, recv_sem, w_send, w_recv, dp_send, dp_recv, p_send, p_recv,
                o_send, o_recv, d_send, d_recv, g_send, g_recv):
    num_rows, out_len, head_dim = k_buf.shape
    n_steps, _, model_dim = x_in.shape
    slots = k_in.shape[2]
    seq_len = slots * n_tp
    chips = n_tp // CORES
    far = chips // 2
    half_steps = n_steps // CORES
    band = num_rows // BANDS
    band_rows = half_steps * band
    piece_steps = half_steps // CUTS
    piece = piece_steps * band
    wide = CORES * head_dim
    n_groups = num_rows // GROUP_ROWS
    share = model_dim // n_dp
    quarter = model_dim // 4

    dp = lax.axis_index("dp")
    me = lax.axis_index("tp")
    chip = me // CORES
    core = lax.rem(me, CORES)
    other = 1 - core

    def chip_at(offset):
        return lax.rem(chip + offset + chips, chips)

    def device(chip_index, core_index):
        return (dp, chip_index * CORES + core_index)

    def sibling(offset):
        return (lax.rem(dp + offset, n_dp), me)

    partner = device(chip, other)
    offsets = [0] + [s * d for d in range(1, far) for s in (1, -1)] + [far]
    my_lanes = pl.ds(pl.multiple_of(core * head_dim, head_dim), head_dim)

    barrier = pltpu.get_barrier_semaphore()
    for off in offsets:
        for c in range(CORES):
            if (off, c) != (0, 0):
                pl.semaphore_signal(barrier, inc=1, device_id=device(chip_at(off), lax.rem(core + c, CORES)), device_id_type=MESH)
    for off in range(1, n_dp):
        pl.semaphore_signal(barrier, inc=1, device_id=sibling(off), device_id_type=MESH)

    my_share = pl.ds(pl.multiple_of(dp * share, share), share)
    loads = [
        pltpu.make_async_copy(plen_in, plen, in_sem.at[0]),
        pltpu.make_async_copy(w_q, wq_v, in_sem.at[1]),
        pltpu.make_async_copy(w_k, wk_v, in_sem.at[2]),
        pltpu.make_async_copy(w_v, wv_v, in_sem.at[3]),
        pltpu.make_async_copy(w_o.at[:, my_share], w_all.at[chip, my_lanes, my_share], in_sem.at[4]),
        pltpu.make_async_copy(x_in.at[pl.ds(core * half_steps, half_steps)], x_res, in_sem.at[5]),
        pltpu.make_async_copy(w_norm, norm_v, in_sem.at[6]),
        pltpu.make_async_copy(
            x_in.at[pl.ds(other * half_steps, half_steps), pl.ds((BANDS - 1) * band, band)], x_oth, in_sem.at[7]),
    ]
    for load in loads:
        load.start()

    def x_load(i, slot):
        return pltpu.make_async_copy(x_in.at[pl.ds(i * X_STEPS, X_STEPS)], x_blk.at[slot], x_sem.at[slot])

    x_load(0, 0).start()

    with jax.named_scope("barrier"):
        pl.semaphore_wait(barrier, n_tp - 1 + n_dp - 1)

    def hops(way, j):
        return far if (way + j) % 2 == 0 else far - 1

    def ring_copy(at, sems, way, hop, j, first=None):
        step = 1 if way == 0 else -1
        view = at(chip_at(-step * (hop - 1)), j)
        return pltpu.make_async_remote_copy(
            src_ref=view if first is None else first, dst_ref=view,
            send_sem=sems[0], recv_sem=sems[1].at[way, hop - 1, j],
            device_id=device(chip_at(step), core), device_id_type=MESH)

    def legs(hop, pieces):
        by_way = [sorted(pieces, key=lambda j, way=way: -hops(way, j)) for way in range(2)]
        return [(way, js[way]) for js in zip(*by_way) for way in range(2) if hop <= hops(way, js[way])]

    def ring_turn(at, sems, hop, pieces, then=None):
        for way, j in legs(hop, pieces):
            ring_copy(at, sems, way, hop, j).wait_recv()
            if hop < hops(way, j):
                ring_copy(at, sems, way, hop + 1, j).start()
            if then is not None:
                then(chip_at(-hop if way == 0 else hop), j)

    def wait_bytes(view, sem):
        pltpu.make_async_copy(view, view, sem).wait()

    w_half = head_dim // 2
    w_sems = (w_send, w_recv)

    def w_at(c, j):
        return w_all.at[c, pl.ds(pl.multiple_of(core * head_dim, head_dim) + j * w_half, w_half), my_share]

    for way, j in legs(1, range(2)):
        ring_copy(w_at, w_sems, way, 1, j, w_o.at[pl.ds(j * w_half, w_half), my_share]).start()

    my_slots = pl.ds(pl.multiple_of(me * slots, slots), slots)

    def send_group(i, _):
        rows = pl.ds(i * GROUP_ROWS, GROUP_ROWS)
        for which, (src, dst) in enumerate(((k_in, k_buf), (v_in, v_buf))):
            pltpu.make_async_copy(src.at[rows, me], dst.at[rows, my_slots], recv_sem.at[which, i]).start()
            for c in range(CORES):
                for off in reversed(offsets):
                    if (off, c) != (0, 0):
                        to_core = lax.rem(core + c, CORES)
                        to_chip = chip_at(off)
                        pltpu.make_async_remote_copy(
                            src_ref=src.at[rows, to_chip * CORES + to_core],
                            dst_ref=dst.at[rows, my_slots],
                            send_sem=send_sem.at[which],
                            recv_sem=recv_sem.at[which, i],
                            device_id=device(to_chip, to_core),
                            device_id_type=MESH,
                        ).start()
        return 0

    send_group(0, 0)

    for load in (*loads[:4], loads[6]):
        load.wait()
    gain[...] = 1.0 + norm_v[...].astype(F32).reshape(1, model_dim)
    n_blocks = n_steps // X_STEPS
    blk_rows = X_STEPS * num_rows

    def project(i, _):
        slot = lax.rem(i, 2)

        @pl.when(i + 1 < n_blocks)
        def _():
            x_load(i + 1, 1 - slot).start()

        x_load(i, slot).wait()
        x = x_blk[slot].reshape(blk_rows, model_dim).astype(F32)
        inv = lax.rsqrt(jnp.mean(x * x, axis=-1, keepdims=True) + NORM_EPS)
        normed = (x * inv * gain[...]).astype(BF16)
        out = pl.ds(pl.multiple_of(i * blk_rows, blk_rows), blk_rows)
        for j, w in enumerate((wq_v, wk_v, wv_v)):
            qkv[j, out, :] = jnp.dot(normed, w[...], preferred_element_type=F32).astype(BF16).astype(F32)
        return 0

    with jax.named_scope("project"):
        lax.fori_loop(0, n_blocks, project, 0)

    with jax.named_scope("w_hop1"):
        ring_turn(w_at, w_sems, 1, range(2))
    send_group(1, 0)

    def rope_row(b, _):
        step_id = lax.broadcasted_iota(jnp.int32, (n_steps, head_dim), 0)
        angle = (step_id + plen[b]).astype(F32) * freq[...]
        lane = lax.broadcasted_iota(jnp.int32, (n_steps, head_dim), 1)
        cos_part = jnp.cos(angle)
        sin_part = jnp.where(lane < head_dim // 2, -1.0, 1.0) * jnp.sin(angle)
        row = pl.ds(b, n_steps, stride=num_rows)

        def rotate(u):
            return u * cos_part + pltpu.roll(u, head_dim // 2, 1) * sin_part

        q_s[b] = (rotate(qkv[0, row, :]) * head_dim ** -0.5).astype(BF16)
        k_n[b] = rotate(qkv[1, row, :]).astype(BF16)
        v_n[b] = qkv[2, row, :].astype(BF16)
        for buf in (k_buf, v_buf):
            buf[b, seq_len:, :] = jnp.zeros((out_len - seq_len, head_dim), BF16)
        return 0

    with jax.named_scope("rope"):
        lax.fori_loop(0, num_rows, rope_row, 0)

    for hop in range(2, far):
        with jax.named_scope(f"w_hop{hop}"):
            ring_turn(w_at, w_sems, hop, range(2))
        send_group(hop, 0)
    with jax.named_scope(f"w_hop{far}"):
        ring_turn(w_at, w_sems, far, range(2))
    loads[4].wait()

    def to_sibling(off):
        view = w_all.at[:, my_lanes, my_share]
        return pltpu.make_async_remote_copy(
            src_ref=view, dst_ref=view, send_sem=dp_send, recv_sem=dp_recv,
            device_id=sibling(off), device_id_type=MESH)

    others_share = w_all.at[:, pl.ds(0, head_dim), pl.ds(0, (n_dp - 1) * share)]
    for off in range(1, n_dp):
        to_sibling(off).start()
    lax.fori_loop(far, n_groups, send_group, 0)

    w_swap = pltpu.make_async_remote_copy(
        src_ref=w_all.at[:, my_lanes], dst_ref=w_all.at[:, my_lanes], send_sem=p_send.at[BANDS], recv_sem=p_recv.at[BANDS],
        device_id=partner, device_id_type=MESH)

    def attend_row(b):
        start = plen[b]
        slot_id = lax.broadcasted_iota(jnp.int32, (out_len, n_steps), 0)
        step_id = lax.broadcasted_iota(jnp.int32, (out_len, n_steps), 1)
        pick = jnp.where(slot_id - step_id == start, 1.0, 0.0).astype(BF16)
        at = lax.broadcasted_iota(jnp.int32, (out_len, head_dim), 0) - start
        is_new = jnp.logical_and(at >= 0, at < n_steps)
        for buf, new in ((k_buf, k_n), (v_buf, v_n)):
            placed = jnp.dot(pick, new[b], preferred_element_type=F32)
            buf[b] = jnp.where(is_new, placed, buf[b].astype(F32)).astype(BF16)
        s = lax.dot_general(q_s[b], k_buf[b], (((1,), (1,)), ((), ())), preferred_element_type=F32)
        s_slot = lax.broadcasted_iota(jnp.int32, (n_steps, out_len), 1)
        s_step = lax.broadcasted_iota(jnp.int32, (n_steps, out_len), 0)
        s = jnp.where(s_slot - s_step <= start, s, -jnp.inf)
        e = jnp.exp(s - jnp.max(s, axis=-1, keepdims=True))
        a = (e / jnp.sum(e, axis=-1, keepdims=True)).astype(BF16)
        o = jnp.dot(a, v_buf[b], preferred_element_type=F32)
        o_sr[b // band, pl.ds(lax.rem(b, band), n_steps, stride=band), :] = o.astype(BF16).astype(F32)

    mine = pl.ds(pl.multiple_of(core * band_rows, band_rows), band_rows)
    theirs = pl.ds(pl.multiple_of(other * band_rows, band_rows), band_rows)
    o_sems = (o_send, o_recv)

    def swap(h):
        return pltpu.make_async_remote_copy(
            src_ref=o_snd.at[h], dst_ref=o_all.at[chip, pl.ds(h * band_rows, band_rows), my_lanes],
            send_sem=p_send.at[h], recv_sem=p_recv.at[h], device_id=partner, device_id_type=MESH)

    def swap_start(h):
        o_snd[h] = o_sr[h, theirs, :].astype(BF16)
        swap(h).start()
        o_all[chip, h * band_rows:(h + 1) * band_rows, my_lanes] = o_sr[h, mine, :].astype(BF16)

    def o_at(c, j):
        return o_all.at[c, pl.ds(j * piece, piece)]

    def band_pieces(h):
        return range(h * CUTS, (h + 1) * CUTS)

    def o_start(h):
        swap_start(h)
        for way, j in legs(1, band_pieces(h)):
            view = o_all.at[chip, pl.ds(j * piece, piece), my_lanes]
            for to_core, src in ((core, view), (other, o_snd.at[h, pl.ds(j % CUTS * piece, piece)])):
                pltpu.make_async_remote_copy(
                    src_ref=src, dst_ref=view, send_sem=o_send, recv_sem=o_recv.at[way, 0, j],
                    device_id=device(chip_at(1 if way == 0 else -1), to_core), device_id_type=MESH).start()

    def attend_group(i, _):
        rows = pl.ds(i * GROUP_ROWS, GROUP_ROWS)
        with jax.named_scope("wait_group"):
            for which, buf in enumerate((k_buf, v_buf)):
                wait_bytes(buf.at[rows, pl.ds(0, seq_len)], recv_sem.at[which, i])
        with jax.named_scope("attend_group"):
            for r in range(GROUP_ROWS):
                attend_row(i * GROUP_ROWS + r)

        @pl.when(i == n_groups // 2 - 1)
        def _():
            o_start(0)

        @pl.when(i == n_groups - 3)
        def _():
            if n_dp > 1:
                wait_bytes(others_share, dp_recv)
            w_swap.start()

        return 0

    lax.fori_loop(0, n_groups, attend_group, 0)

    def y_view(of_core, h, cols):
        return y_buf.at[pl.ds(pl.multiple_of(of_core * half_steps, half_steps), half_steps), pl.ds(h * band, band), cols]

    def hand_on(of_core, h, q):
        view = y_view(of_core, h, pl.ds(q * quarter, quarter))
        return pltpu.make_async_remote_copy(
            src_ref=view, dst_ref=view, send_sem=d_send.at[h], recv_sem=d_recv.at[h],
            device_id=partner, device_id_type=MESH)

    def y_add(h, froms, first=False, last=False):
        passed = h == BANDS
        rows = slice(0, band_rows) if passed else slice(h * band_rows, (h + 1) * band_rows)
        o_ref = o_oth if passed else o_all
        for n in range(model_dim // wide):
            cols = slice(n * wide, (n + 1) * wide)
            total = None
            for off in froms:
                c = chip_at(off)
                part = jnp.dot(o_ref[c, rows, :], w_all[c, :, cols], preferred_element_type=F32)
                total = part if total is None else total + part
            if first:
                x = x_oth[:, :, cols] if passed else x_res[:, h * band:(h + 1) * band, cols]
                total += x.astype(F32).reshape(band_rows, wide)
            else:
                total += y_acc[h, :, cols]
            if last:
                y_view(other if passed else core, min(h, BANDS - 1), pl.ds(n * wide, wide))[...] = total.reshape(half_steps, band, wide).astype(BF16)
                if h < BANDS - 1 and (n + 1) * wide % quarter == 0:
                    hand_on(core, h, n * wide // quarter).start()
            else:
                y_acc[h, :, cols] = total

    def pass_on(stage):
        def start(c, j):
            pltpu.make_async_remote_copy(
                src_ref=o_all.at[c, pl.ds(j * piece, piece)], dst_ref=o_oth.at[c, pl.ds(j % CUTS * piece, piece)],
                send_sem=g_send, recv_sem=g_recv.at[stage], device_id=partner, device_id_type=MESH).start()
        return start

    near = [s * d for d in range(1, far - 1) for s in (1, -1)]
    edge = [far - 1, 1 - far]

    def turn(h, hop):
        with jax.named_scope(f"o_b{h}_hop{hop}"):
            then = pass_on(max(0, hop - far + 2)) if h == BANDS - 1 else None
            ring_turn(o_at, o_sems, hop, band_pieces(h), then)

    def add(h, froms, **kwargs):
        with jax.named_scope(f"y_b{h}"):
            if h == BANDS:
                stage = 0 if "first" in kwargs else 2 if "last" in kwargs else 1
                wait_bytes(o_oth.at[pl.ds(0, len(froms))], g_recv.at[stage])
            y_add(h, froms, **kwargs)

    o_start(1)
    turn(0, 1)
    turn(1, 1)
    for hop in range(2, far + 1):
        turn(0, hop)
        if hop == far - 2:
            loads[5].wait()
            loads[7].wait()
            w_swap.wait_recv()
            for h in range(BANDS):
                swap(h).wait_recv()
            for j in band_pieces(1):
                pass_on(0)(chip, j)
            add(0, [0] + near, first=True)
        if hop == far - 1:
            add(0, edge)
            add(2, [0] + near, first=True)
        if hop == far:
            add(0, [far], last=True)
        turn(1, hop)
        if hop == far - 2:
            add(1, [0] + near, first=True)
        if hop == far - 1:
            add(1, edge)
    for stage, count in ((1, 2), (2, 1)):
        wait_bytes(o_oth.at[pl.ds(0, count)], g_recv.at[stage])

    with jax.named_scope("drain"):
        for which, buf in enumerate((k_buf, v_buf)):
            wait_bytes(buf.at[:, pl.ds(0, seq_len - slots)], send_sem.at[which])
        wait_bytes(w_all.at[pl.ds(0, chips - 1), pl.ds(0, head_dim), pl.ds(0, share)], w_send)
        wait_bytes(o_all.at[pl.ds(0, chips - 1)], o_send)
        if n_dp > 1:
            wait_bytes(others_share, dp_send)
        w_swap.wait_send()
        for h in range(BANDS):
            swap(h).wait_send()
        for h in range(BANDS - 1):
            wait_bytes(y_view(core, h, pl.ds(0, model_dim)), d_send.at[h])
            wait_bytes(y_view(other, h, pl.ds(0, model_dim)), d_recv.at[h])
        wait_bytes(o_oth, g_send)


def write_kernel(k_buf, v_buf, y_buf, o_all, w_all, o_oth, y_acc, k_out, v_out, y_out, y_last, sem, y_sem):
    n_steps, num_rows, model_dim = y_buf.shape
    chips, band_rows, wide = o_oth.shape
    half_steps, band = n_steps // CORES, num_rows // BANDS
    me = lax.axis_index("tp")
    core = lax.rem(me, CORES)
    far = chips // 2
    late = [lax.rem(me // CORES + off + chips, chips) for off in (far, far - 1, 1 - far)]
    parts = sem.shape[1]
    copies = []
    for a, (src, dst) in enumerate(((k_buf, k_out), (v_buf, v_out))):
        size = src.shape[0] // parts
        for i in range(parts):
            copies.append(pltpu.make_async_copy(src.at[pl.ds(i * size, size)], dst.at[pl.ds(i * size, size)], sem.at[a, i]))
    done = pl.ds(0, num_rows - band)
    copies.append(pltpu.make_async_copy(y_buf.at[:, done], y_out.at[:, done], y_sem.at[CORES]))
    for copy in copies:
        copy.start()

    rest = pl.ds(num_rows - band, band)
    for half in range(CORES):
        of_core = lax.rem(core + half, CORES)
        steps = pl.ds(pl.multiple_of(of_core * half_steps, half_steps), half_steps)
        for n in range(model_dim // wide):
            cols = slice(n * wide, (n + 1) * wide)
            total = y_acc[BANDS - 1 + half, :, cols]
            for c in (late if half else late[:1]):
                o = o_oth[c] if half else o_all[c, (BANDS - 1) * band_rows:, :]
                total += jnp.dot(o, w_all[c, :, cols], preferred_element_type=F32)
            y_last[half, :, :, cols] = total.reshape(half_steps, band, wide).astype(BF16)
        copies.append(pltpu.make_async_copy(y_last.at[half], y_out.at[steps, rest], y_sem.at[half]))
        copies[-1].start()
    for copy in copies:
        copy.wait()


def solution(mesh):
    n_tp = mesh.shape["tp"]
    n_dp = mesh.shape["dp"]

    def local_block(k_cache, v_cache, prompt_len, x_steps, w_norm, w_q, w_k, w_v, w_o):
        num_rows, _, slots, head_dim = k_cache.shape
        n_steps, _, model_dim = x_steps.shape
        out_len = slots * n_tp + n_steps
        chips = n_tp // CORES
        far = chips // 2
        half_steps = n_steps // CORES
        half_rows = half_steps * num_rows
        wide = CORES * head_dim
        n_groups = num_rows // GROUP_ROWS
        pieces = BANDS * CUTS
        lanes = jnp.arange(head_dim, dtype=jnp.int32) % (head_dim // 2)
        freq = (ROPE_BASE ** (-2.0 * lanes.astype(F32) / head_dim)).reshape(1, head_dim)
        dma = pltpu.SemaphoreType.DMA
        in_hbm = functools.partial(pltpu.with_memory_space_constraint, memory_space=pltpu.HBM)

        def in_vmem(shape):
            return pltpu.VMEM(shape.shape, shape.dtype)

        hbm = pl.BlockSpec(memory_space=pltpu.HBM)
        vmem = pl.BlockSpec(memory_space=pltpu.VMEM)
        cache = jax.ShapeDtypeStruct((num_rows, out_len, head_dim), BF16)
        y_shape = jax.ShapeDtypeStruct(x_steps.shape, BF16)
        rest = (
            jax.ShapeDtypeStruct((chips, half_rows, wide), BF16),
            jax.ShapeDtypeStruct((chips, wide, model_dim), BF16),
            jax.ShapeDtypeStruct((chips, half_rows // BANDS, wide), BF16),
            jax.ShapeDtypeStruct((BANDS + 1, half_rows // BANDS, model_dim), F32),
        )
        bufs = pl.pallas_call(
            functools.partial(main_kernel, n_tp, n_dp),
            out_shape=tuple(map(in_vmem, (cache, cache, y_shape, *rest))),
            in_specs=[hbm, vmem] + [hbm] * 8,
            out_specs=(vmem,) * 7,
            scratch_shapes=[
                pltpu.SMEM(prompt_len.shape, jnp.int32),
                pltpu.VMEM(w_norm.shape, BF16),
                pltpu.VMEM((1, model_dim), F32),
                pltpu.VMEM((model_dim, head_dim), BF16),
                pltpu.VMEM((model_dim, head_dim), BF16),
                pltpu.VMEM((model_dim, head_dim), BF16),
                pltpu.VMEM((2, X_STEPS, num_rows, model_dim), BF16),
                pltpu.VMEM((3, n_steps * num_rows, head_dim), F32),
                pltpu.VMEM((num_rows, n_steps, head_dim), BF16),
                pltpu.VMEM((num_rows, n_steps, head_dim), BF16),
                pltpu.VMEM((num_rows, n_steps, head_dim), BF16),
                pltpu.VMEM((BANDS, n_steps * num_rows // BANDS, head_dim), F32),
                pltpu.VMEM((BANDS, half_rows // BANDS, head_dim), BF16),
                pltpu.VMEM((half_steps, num_rows, model_dim), BF16),
                pltpu.VMEM((half_steps, num_rows // BANDS, model_dim), BF16),
                dma((8,)), dma((2,)),
                dma((2,)), dma((2, n_groups)),
                dma, dma((2, far, 2)),
                dma, dma,
                dma((BANDS + 1,)), dma((BANDS + 1,)),
                dma, dma((2, far, pieces)),
                dma((BANDS,)), dma((BANDS,)),
                dma, dma((3,)),
            ],
            compiler_params=pltpu.CompilerParams(collective_id=0, has_side_effects=True, vmem_limit_bytes=24 * 2**20),
            name="decode_block",
        )(in_hbm(prompt_len), freq, *map(in_hbm, (w_norm, k_cache, v_cache, x_steps, w_q, w_k, w_v, w_o)))
        k_out, v_out, y_out = pl.pallas_call(
            write_kernel,
            out_shape=(cache, cache, y_shape),
            in_specs=[vmem] * 7,
            out_specs=(hbm, hbm, hbm),
            scratch_shapes=[pltpu.VMEM((CORES, half_steps, num_rows // BANDS, model_dim), BF16), dma((2, 8)), dma((CORES + 1,))],
            compiler_params=pltpu.CompilerParams(vmem_limit_bytes=8 * 2**20),
            name="write_out",
        )(*bufs)
        return y_out, k_out[:, None], v_out[:, None]

    cache_spec = P("dp", None, "tp", None)
    col_spec = P(None, "tp")
    out_cache_spec = P("dp", "tp", None, None)
    return jax.shard_map(local_block, mesh=mesh, in_specs=(cache_spec, cache_spec, P("dp"), P(None, "dp", None), P(None), col_spec, col_spec, col_spec, P("tp", None)), out_specs=(P(None, "dp", None), out_cache_spec, out_cache_spec), check_vma=False)
```
